128 devices in a mesh: tm: 16 (over z_lo, y, core), chan: 8 (over x, z_hi).
Axes of the slice: x: 4, y: 4, z: 4 (z_hi: 2, z_lo: 2; z = z_hi * 2 + z_lo), core: 2. Of those that a mesh axis runs over, the one named last changes fastest.
Arguments:
- auxiliary: float32 [512, 524288], P('chan', 'tm'), may hold values from -30 to 30
- proofs: float32 [64, 524288], P('chan', 'tm'), may hold values from -12 to 12
Outputs:
- coherence: float32 [512, 64, 4096], P('chan', None, 'tm')
The draws below stay inside these ranges and needn't reach their ends.
All inputs are finite; a program needn't handle non-finite values.
Results may differ from the reference program's by a relative error of at most 0.00076.
Values may be sent and summed in bfloat16 or wider, within the bound.
A program may use at most 192 MiB of HBM per device.

```python
import math
import jax
import jax.numpy as jnp
from jax import lax

AUX_CH = 512
WIT_CH = 64
SEG_LEN = 8192
STRIDE = 4096
BINS = 4096
SEGMENTS = 127
SAMPLES = 524288


def coupled_series(key):
    subkeys = [jax.random.fold_in(key, 101 + number) for number in range(9)]
    moments = jnp.arange(SAMPLES, dtype=jnp.float32) / SAMPLES
    wit_noise = jax.random.truncated_normal(subkeys[0], -6.0, 6.0, (WIT_CH, SAMPLES), jnp.float32)
    aux_noise = jax.random.truncated_normal(subkeys[1], -6.0, 6.0, (AUX_CH, SAMPLES), jnp.float32)
    spread = 1.0
    wit_offset = jax.random.uniform(subkeys[2], (WIT_CH,), jnp.float32, -spread, spread)
    proof_out = wit_noise + wit_offset[:, None] * (0.5 + moments)[None, :]
    target = jax.random.randint(subkeys[3], (AUX_CH,), 0, WIT_CH)
    delays = jax.random.randint(subkeys[4], (AUX_CH,), 0, 4)
    gains_aux = jax.random.uniform(subkeys[5], (AUX_CH,), jnp.float32, 0.0, 2.0)
    source = wit_noise[target]
    shifted = jax.vmap(lambda series_row, amount: jnp.roll(series_row, amount))(source, delays)
    aux_offset = jax.random.uniform(subkeys[6], (AUX_CH,), jnp.float32, -spread, spread)
    aux_out = aux_noise + gains_aux[:, None] * shifted + aux_offset[:, None] * (1.0 + 2.0 * moments)[None, :]
    return (aux_out, proof_out)


def draw_auxiliary(key, part):
    return coupled_series(key)[0]


def draw_proofs(key, part):
    return coupled_series(key)[1]


def setup_inputs(seed: int = 0) -> dict:
    seeds = jax.random.split(jax.random.key(seed), 3)
    auxiliary = draw_auxiliary(jax.random.fold_in(seeds[2], 71), 0)
    proofs = draw_proofs(jax.random.fold_in(seeds[2], 71), 0)
    return dict(auxiliary=auxiliary, proofs=proofs)


def spectra_of(series, channel_means):
    row_count = series.shape[0]
    blocks = series.reshape(row_count, SEGMENTS + 1, STRIDE)
    segments = jnp.concatenate([blocks[:, :-1], blocks[:, 1:]], axis=2)
    position = jnp.arange(SEG_LEN, dtype=jnp.float32)
    window = 0.5 - 0.5 * jnp.cos(2.0 * math.pi * position / SEG_LEN)
    windowed = (segments - channel_means[:, None, None]) * window
    spectrum = jnp.fft.rfft(windowed, axis=-1)[..., :BINS]
    return jnp.real(spectrum).astype(jnp.bfloat16), jnp.imag(spectrum).astype(jnp.bfloat16)


def reference(auxiliary, proofs):
    aux_means = jnp.sum(auxiliary, axis=1) / SAMPLES
    wit_means = jnp.sum(proofs, axis=1) / SAMPLES
    wit_real, wit_imag = spectra_of(proofs, wit_means)
    wit_real = wit_real.astype(jnp.float32)
    wit_imag = wit_imag.astype(jnp.float32)
    wit_power = jnp.sum(wit_real * wit_real + wit_imag * wit_imag, axis=1)
    block_size = math.gcd(AUX_CH, 8)
    aux_blocks = auxiliary.reshape(AUX_CH // block_size, block_size, SAMPLES)
    mean_blocks = aux_means.reshape(AUX_CH // block_size, block_size)

    def one_block(block_pair):
        rows_here, block_means = block_pair
        aux_real, aux_imag = spectra_of(rows_here, block_means)
        aux_real = aux_real.astype(jnp.float32)
        aux_imag = aux_imag.astype(jnp.float32)
        cross_real = jnp.einsum("csf,wsf->cwf", aux_real, wit_real) + jnp.einsum("csf,wsf->cwf", aux_imag, wit_imag)
        cross_imag = jnp.einsum("csf,wsf->cwf", aux_imag, wit_real) - jnp.einsum("csf,wsf->cwf", aux_real, wit_imag)
        aux_power = jnp.sum(aux_real * aux_real + aux_imag * aux_imag, axis=1)
        return (cross_real * cross_real + cross_imag * cross_imag) / ((aux_power[:, None, :] + 1e-6) * (wit_power[None, :, :] + 1e-6))

    result = lax.map(one_block, (aux_blocks, mean_blocks))
    return result.reshape(AUX_CH, WIT_CH, BINS)
```

```python
import math
import functools
import numpy as np
import jax
import jax.numpy as jnp
from jax import lax
from jax.sharding import PartitionSpec as P
from jax.experimental import pallas as pl
from jax.experimental.pallas import tpu as pltpu

NT = (((1,), (1,)), ((), ()))
PITCH = 72


def split(x):
    hi = x.astype(jnp.bfloat16)
    lo = (x - hi.astype(jnp.float32)).astype(jnp.bfloat16)
    return hi, lo


def np_split(x):
    x = jnp.asarray(x, jnp.float32)
    return split(x)


def fft_tables():
    a = np.arange(64)
    ang = 2 * np.pi * np.outer(a, a) % (2 * np.pi * 64) / 64
    ang = 2 * np.pi * (np.outer(a, a) % 64) / 64
    f1 = np.concatenate([np.cos(ang), -np.sin(ang)], 0)
    h, l = np_split(f1)
    f1cat = jnp.concatenate([h, h, l, l], axis=1)
    lane = np.arange(128)
    k2 = np.arange(32)
    ang2 = 2 * np.pi * (np.outer(k2, lane) % 64) / 64
    re = np.concatenate([np.cos(ang2), np.sin(ang2)], 1)
    im = np.concatenate([-np.sin(ang2), np.cos(ang2)], 1)
    h, l = np_split(np.concatenate([re, im], 0))
    w2 = jnp.concatenate([h, l], axis=0)
    k1 = np.arange(128)
    angt = 2 * np.pi * (np.outer(k1, lane) % 8192) / 8192
    cos_t = jnp.asarray(np.cos(angt), jnp.float32)
    sin_t = jnp.asarray(np.sin(angt), jnp.float32)
    n = np.arange(8192)
    hann = jnp.asarray((0.5 - 0.5 * np.cos(2 * np.pi * n / 8192)).reshape(64, 128), jnp.float32)
    return f1cat, w2, cos_t, sin_t, hann


def fft_step(x2d, base, mean8, scr, s, tabs):
    f1, w2, cos_t, sin_t, hann = tabs
    cats = []
    for c in range(8):
        xs = (x2d[pl.ds(base + s * 256 + c, 64, stride=8), :] - mean8[c:c + 1]) * hann[...]
        h, l = split(xs)
        cats.append(jnp.concatenate([h, l, h, l], axis=0))
    y = jnp.dot(f1[...], jnp.concatenate(cats, axis=1), preferred_element_type=jnp.float32)
    zh, zl = [], []
    for c in range(8):
        yre = y[:64, 128 * c:128 * c + 128]
        yim = y[64:, 128 * c:128 * c + 128]
        for b in range(2):
            ct = cos_t[64 * b:64 * b + 64]
            st = sin_t[64 * b:64 * b + 64]
            h, l = split(jnp.concatenate([yre * ct + yim * st, yim * ct - yre * st], axis=1))
            zh.append(h)
            zl.append(l)
    w = w2[...]
    a = lax.dot_general(w, jnp.concatenate(zh, axis=0), NT, preferred_element_type=jnp.float32)
    b = lax.dot_general(w[:64], jnp.concatenate(zl, axis=0), NT, preferred_element_type=jnp.float32)
    o = a[:64] + a[64:] + b
    for c in range(8):
        scr[pl.ds(c * 8 + s, 64, stride=PITCH), :] = o[:, 128 * c:128 * c + 128]


def spectra_kernel(peers, aux, wit, f1, w2, cos_t, sin_t, hann, recv, x, scr, send, sums, means,
                   load_sem, halo_send, halo_recv, sum_send, sum_recv, send_sem, recv_sem, own_sem):
    tabs = (f1, w2, cos_t, sin_t, hann)
    me = lax.axis_index("tm")
    before = lax.rem(me + peers - 1, peers)
    blocks = x.shape[0]

    def source(b):
        return wit.at[0] if b == 0 else aux.at[b - 1]

    loads = []
    for b in range(blocks):
        cp = pltpu.make_async_copy(source(b), x.at[b, pl.ds(0, 256)], load_sem.at[b])
        cp.start()
        loads.append(cp)
    barrier = pltpu.get_barrier_semaphore()

    def greet(j, _):
        pl.semaphore_signal(barrier, inc=1, device_id={"tm": lax.rem(me + j, peers)},
                            device_id_type=pl.DeviceIdType.MESH)
        return 0

    lax.fori_loop(1, peers, greet, 0)
    pl.semaphore_wait(barrier, peers - 1)

    halos = []
    for b in range(blocks):
        cp = pltpu.make_async_remote_copy(
            src_ref=source(b).at[pl.ds(0, 32)], dst_ref=x.at[b, pl.ds(256, 32)],
            send_sem=halo_send.at[b], recv_sem=halo_recv.at[b],
            device_id={"tm": before}, device_id_type=pl.DeviceIdType.MESH)
        cp.start()
        halos.append(cp)

    lane = lax.broadcasted_iota(jnp.int32, (8, 128), 1)
    total = jnp.zeros((8, 128), jnp.float32)
    for b in range(blocks):
        loads[b].wait()

        def add(i, acc):
            return acc + jnp.sum(x[b, pl.ds(i * 16, 16)], axis=0)

        part = lax.fori_loop(0, 16, add, jnp.zeros((8, 128), jnp.float32))
        total = jnp.where(lane == b, jnp.sum(part, axis=1, keepdims=True), total)
    sums[0] = total

    def sum_copy(j):
        return pltpu.make_async_remote_copy(
            src_ref=sums.at[0], dst_ref=sums.at[j], send_sem=sum_send.at[j], recv_sem=sum_recv.at[j],
            device_id={"tm": lax.rem(me + j, peers)}, device_id_type=pl.DeviceIdType.MESH)

    def sum_start(j, _):
        sum_copy(j).start()
        return 0

    def sum_wait(j, acc):
        sum_copy(j).wait()
        return acc + sums[j]

    lax.fori_loop(1, peers, sum_start, 0)
    total = lax.fori_loop(1, peers, sum_wait, total)
    mean = total / (256 * 128 * peers)
    for b in range(blocks):
        means[b] = jnp.broadcast_to(mean[:, b:b + 1], (8, 128))
    for b in range(blocks):
        halos[b].wait()

    x2d = x.reshape(blocks * 288 * 8, 128)
    row = lax.broadcasted_iota(jnp.int32, (64, 128), 0)
    keep = jnp.where((lax.rem(row, 8) == 7) & (me == peers - 1), 0.0, 1.0)

    def block_copy(b, j):
        slot = lax.rem(b, 2)
        to = lax.rem(me + j, peers)
        return pltpu.make_async_remote_copy(
            src_ref=send.at[slot, to], dst_ref=recv.at[b, me],
            send_sem=send_sem.at[slot, j], recv_sem=recv_sem.at[b, j],
            device_id={"tm": to}, device_id_type=pl.DeviceIdType.MESH)

    def own_copy(b):
        slot = lax.rem(b, 2)
        return pltpu.make_async_copy(send.at[slot, me], recv.at[b, me], own_sem.at[slot])

    def drain(b):
        def one(j, _):
            block_copy(b, j).wait_send()
            return 0
        lax.fori_loop(1, peers, one, 0)
        own_copy(b).wait()

    def block(b, _):
        slot = lax.rem(b, 2)
        mean8 = means[b]

        def step(s, _):
            fft_step(x2d, b * 2304, mean8, scr, s, tabs)
            return 0

        lax.fori_loop(0, 8, step, 0)

        @pl.when(b >= 2)
        def _():
            drain(b - 2)

        def pack(d, _):
            for part in range(2):
                for half in range(2):
                    at = pl.multiple_of((part * 32 + d * 2 + half) * PITCH, 8)
                    v = scr[pl.ds(at, 64), :] * keep
                    send[slot, d, part, :, half * 128:half * 128 + 128] = v.astype(jnp.bfloat16)
            return 0

        lax.fori_loop(0, peers, pack, 0)

        def go(j, _):
            block_copy(b, j).start()
            return 0

        lax.fori_loop(1, peers, go, 0)
        own_copy(b).start()
        return 0

    lax.fori_loop(0, blocks, block, 0)
    drain(blocks - 2)
    drain(blocks - 1)

    def landed(b, _):
        def one(j, _):
            block_copy(b, j).wait_recv()
            return 0
        return lax.fori_loop(1, peers, one, 0)

    lax.fori_loop(0, blocks, landed, 0)


def spectra(aux, wit, peers):
    tabs = fft_tables()
    vm = pl.BlockSpec(memory_space=pltpu.VMEM)
    hbm = pl.BlockSpec(memory_space=pl.ANY)
    blocks = aux.shape[0] + 1
    dma = pltpu.SemaphoreType.DMA
    return pl.pallas_call(
        functools.partial(spectra_kernel, peers),
        out_shape=jax.ShapeDtypeStruct((blocks, peers, 2, 64, 256), jnp.bfloat16),
        in_specs=[hbm, hbm] + [vm] * 5,
        out_specs=hbm,
        scratch_shapes=[
            pltpu.VMEM((blocks, 288, 8, 128), jnp.float32),
            pltpu.VMEM((64 * PITCH, 128), jnp.float32),
            pltpu.VMEM((2, peers, 2, 64, 256), jnp.bfloat16),
            pltpu.VMEM((peers, 8, 128), jnp.float32),
            pltpu.VMEM((blocks, 8, 128), jnp.float32),
            dma((blocks,)), dma((blocks,)), dma((blocks,)),
            dma((peers,)), dma((peers,)),
            dma((2, peers)), dma((blocks, peers)), dma((2,)),
        ],
        compiler_params=pltpu.CompilerParams(
            collective_id=0, has_side_effects=True, vmem_limit_bytes=62 * 2 ** 20),
    )(aux, wit, *tabs)


def gather_rows(stage, rows):
    def one(i, _):
        t = i // 2
        part = lax.rem(i, 2)
        v = stage[t, part].astype(jnp.float32)
        at = pl.multiple_of(part * 128 + t * 8, 8)
        for c in range(8):
            rows[c, pl.ds(at, 8), :] = v[8 * c:8 * c + 8]
        return 0
    lax.fori_loop(0, 32, one, 0)


def flip(eye, rows_c):
    return lax.dot_general(eye, rows_c.astype(jnp.bfloat16), NT, preferred_element_type=jnp.float32)


def proof_kernel(recv, eye, out, power, stage, rows, mat_re, mat_im, sem):
    cp = pltpu.make_async_copy(recv.at[0], stage, sem)
    cp.start()
    cp.wait()
    gather_rows(stage, rows)
    for w in range(8):
        r = rows[w]
        power[w:w + 1, :] = jnp.sum(r * r, axis=0, keepdims=True)
        t = flip(eye[...], r)
        mat_re[pl.ds(w, 256, stride=8), :] = t[:, :128]
        mat_im[pl.ds(w, 256, stride=8), :] = t[:, 128:]

    def one(f, _):
        at = pl.ds(pl.multiple_of(f * 8, 8), 8)
        out[f] = jnp.concatenate([mat_re[at, :], mat_im[at, :]], axis=1).astype(jnp.bfloat16)
        return 0
    lax.fori_loop(0, 256, one, 0)


def proof_matrix(recv, eye):
    vm = pl.BlockSpec(memory_space=pltpu.VMEM)
    return pl.pallas_call(
        proof_kernel,
        out_shape=(jax.ShapeDtypeStruct((256, 8, 256), jnp.bfloat16),
                   jax.ShapeDtypeStruct((8, 256), jnp.float32)),
        in_specs=[pl.BlockSpec(memory_space=pl.ANY), vm],
        out_specs=(vm, vm),
        scratch_shapes=[
            pltpu.VMEM((16, 2, 64, 256), jnp.bfloat16),
            pltpu.VMEM((8, 256, 256), jnp.float32),
            pltpu.VMEM((256 * 8, 128), jnp.float32),
            pltpu.VMEM((256 * 8, 128), jnp.float32),
            pltpu.SemaphoreType.DMA,
        ],
        compiler_params=pltpu.CompilerParams(vmem_limit_bytes=62 * 2 ** 20),
    )(recv, eye)


def coherence_kernel(recv, wmat, wpow, eye, out, stage, rows, mat_re, mat_im, wv, apow, tile, load_sem, w_sem, out_sem):
    wcp = pltpu.make_async_copy(wmat, wv, w_sem)
    wcp.start()

    def load(b):
        return pltpu.make_async_copy(recv.at[b + 1], stage.at[lax.rem(b, 2)], load_sem.at[lax.rem(b, 2)])

    load(0).start()

    def block(b, _):
        @pl.when(b < 7)
        def _():
            load(b + 1).start()
        load(b).wait()
        gather_rows(stage.at[lax.rem(b, 2)], rows)
        e = eye[...]
        for c in range(8):
            r = rows[c]
            apow[b, c:c + 1, :] = jnp.sum(r * r, axis=0, keepdims=True)
            t = flip(e, r)
            mat_re[pl.ds(b * 8 + c, 256, stride=PITCH), :] = t[:, :128]
            mat_im[pl.ds(b * 8 + c, 256, stride=PITCH), :] = t[:, 128:]
        return 0

    lax.fori_loop(0, 8, block, 0)
    wcp.wait()

    def bins(i, _):
        for u in range(8):
            f = i * 8 + u
            at = pl.ds(pl.multiple_of(f * PITCH, 8), 64)
            are, aim = mat_re[at, :], mat_im[at, :]
            left = jnp.concatenate([
                jnp.concatenate([are, aim], axis=1),
                jnp.concatenate([aim, -are], axis=1)], axis=0).astype(jnp.bfloat16)
            g = lax.dot_general(left, wv[f], NT, preferred_element_type=jnp.float32)
            mat_re[at, 0:64] = g[:64] * g[:64] + g[64:] * g[64:]
        return 0

    lax.fori_loop(0, 32, bins, 0)

    def store(b):
        return pltpu.make_async_copy(tile.at[lax.rem(b, 2)], out.at[pl.ds(b * 8, 8)], out_sem.at[lax.rem(b, 2)])

    def finish(b, _):
        @pl.when(b >= 2)
        def _():
            store(b - 2).wait()
        for c in range(8):
            for h in range(2):
                num = mat_re[pl.ds(h * 128 * PITCH + b * 8 + c, 128, stride=PITCH), :].T
                cols = slice(128 * h, 128 * h + 128)
                den = (apow[b, c:c + 1, cols] + 1e-06) * (wpow[:, cols] + 1e-06)
                tile[lax.rem(b, 2), c, :, cols] = num[:64] / den
        store(b).start()
        return 0

    lax.fori_loop(0, 8, finish, 0)
    store(6).wait()
    store(7).wait()


def coherence(recv, wmat, wpow, eye):
    vm = pl.BlockSpec(memory_space=pltpu.VMEM)
    hbm = pl.BlockSpec(memory_space=pl.ANY)
    dma = pltpu.SemaphoreType.DMA
    return pl.pallas_call(
        coherence_kernel,
        out_shape=jax.ShapeDtypeStruct((64, 64, 256), jnp.float32),
        in_specs=[hbm, hbm, vm, vm],
        out_specs=hbm,
        scratch_shapes=[
            pltpu.VMEM((2, 16, 2, 64, 256), jnp.bfloat16),
            pltpu.VMEM((8, 256, 256), jnp.float32),
            pltpu.VMEM((256 * PITCH, 128), jnp.float32),
            pltpu.VMEM((256 * PITCH, 128), jnp.float32),
            pltpu.VMEM((256, 64, 256), jnp.bfloat16),
            pltpu.VMEM((8, 8, 256), jnp.float32),
            pltpu.VMEM((2, 8, 64, 256), jnp.float32),
            dma((2,)), dma, dma((2,)),
        ],
        compiler_params=pltpu.CompilerParams(vmem_limit_bytes=62 * 2 ** 20),
    )(recv, wmat, wpow, eye)


def tiles(a):
    return a.reshape(a.shape[0] // 8, 8, 256, 128).transpose(0, 2, 1, 3)


def per_device(auxiliary, proofs):
    peers = lax.axis_size("tm")
    recv = spectra(tiles(auxiliary), tiles(proofs), peers)
    eye = jnp.eye(256, dtype=jnp.bfloat16)
    wpart, wpow = proof_matrix(recv, eye)
    wmat = lax.all_gather(wpart, "chan", axis=1, tiled=True)
    wpow = lax.all_gather(wpow, "chan", axis=0, tiled=True)
    return coherence(recv, wmat, wpow, eye)


def solution(mesh):
    return jax.shard_map(
        per_device,
        mesh=mesh,
        in_specs=(P("chan", "tm"), P("chan", "tm")),
        out_specs=P("chan", None, "tm"),
        check_vma=False,
    )
```

```python
import math
import functools
import numpy as np
import jax
import jax.numpy as jnp
from jax import lax
from jax.sharding import PartitionSpec as P
from jax.experimental import pallas as pl
from jax.experimental.pallas import tpu as pltpu

NT = (((1,), (1,)), ((), ()))
PITCH = 72


def split(x):
    hi = x.astype(jnp.bfloat16)
    lo = (x - hi.astype(jnp.float32)).astype(jnp.bfloat16)
    return hi, lo


def np_split(x):
    x = jnp.asarray(x, jnp.float32)
    return split(x)


def fft_tables():
    a = np.arange(64)
    ang = 2 * np.pi * np.outer(a, a) % (2 * np.pi * 64) / 64
    ang = 2 * np.pi * (np.outer(a, a) % 64) / 64
    f1 = np.concatenate([np.cos(ang), -np.sin(ang)], 0)
    h, l = np_split(f1)
    f1cat = jnp.concatenate([h, h, l, l], axis=1)
    lane = np.arange(128)
    k2 = np.arange(32)
    ang2 = 2 * np.pi * (np.outer(k2, lane) % 64) / 64
    re = np.concatenate([np.cos(ang2), np.sin(ang2)], 1)
    im = np.concatenate([-np.sin(ang2), np.cos(ang2)], 1)
    h, l = np_split(np.concatenate([re, im], 0))
    w2 = jnp.concatenate([h, l], axis=0)
    k1 = np.arange(128)
    angt = 2 * np.pi * (np.outer(k1, lane) % 8192) / 8192
    cos_t = jnp.asarray(np.cos(angt), jnp.float32)
    sin_t = jnp.asarray(np.sin(angt), jnp.float32)
    n = np.arange(8192)
    hann = jnp.asarray((0.5 - 0.5 * np.cos(2 * np.pi * n / 8192)).reshape(64, 128), jnp.float32)
    return f1cat, w2, cos_t, sin_t, hann


def fft_step(x2d, base, mean8, scr, s, tabs):
    f1, w2, cos_t, sin_t, hann = tabs
    cats = []
    for c in range(8):
        xs = (x2d[pl.ds(base + s * 256 + c, 64, stride=8), :] - mean8[c:c + 1]) * hann[...]
        h, l = split(xs)
        cats.append(jnp.concatenate([h, l, h, l], axis=0))
    y = jnp.dot(f1[...], jnp.concatenate(cats, axis=1), preferred_element_type=jnp.float32)
    zh, zl = [], []
    for c in range(8):
        yre = y[:64, 128 * c:128 * c + 128]
        yim = y[64:, 128 * c:128 * c + 128]
        for b in range(2):
            ct = cos_t[64 * b:64 * b + 64]
            st = sin_t[64 * b:64 * b + 64]
            h, l = split(jnp.concatenate([yre * ct + yim * st, yim * ct - yre * st], axis=1))
            zh.append(h)
            zl.append(l)
    w = w2[...]
    a = lax.dot_general(w, jnp.concatenate(zh, axis=0), NT, preferred_element_type=jnp.float32)
    b = lax.dot_general(w[:64], jnp.concatenate(zl, axis=0), NT, preferred_element_type=jnp.float32)
    o = a[:64] + a[64:] + b
    for c in range(8):
        scr[pl.ds(c * 8 + s, 64, stride=PITCH), :] = o[:, 128 * c:128 * c + 128]


def fused_kernel(peers, aux, wit, eye, f1, w2, cos_t, sin_t, hann, num, apow, wpow,
                 x, scr, send, recv, sums, means, rows, mat_re, mat_im, wv, tile,
                 load_sem, halo_send, halo_recv, sum_send, sum_recv, send_sem, recv_sem,
                 ring_send, ring_recv, out_sem):
    tabs = (f1, w2, cos_t, sin_t, hann)
    mesh_id = pl.DeviceIdType.MESH
    me = lax.axis_index("tm")
    mine = lax.axis_index("chan")
    across = mine + 1 - 2 * lax.rem(mine, 2)
    right = lax.rem(mine + 2, 8)
    left = lax.rem(mine + 6, 8)
    before = lax.rem(me + peers - 1, peers)
    blocks = x.shape[0]
    slots = send.shape[0]

    def source(b):
        return wit.at[0] if b == 0 else aux.at[b - 1]

    loads = []
    for b in range(blocks):
        cp = pltpu.make_async_copy(source(b), x.at[b, pl.ds(0, 256)], load_sem.at[b])
        cp.start()
        loads.append(cp)
    barrier = pltpu.get_barrier_semaphore()

    def greet(j, _):
        pl.semaphore_signal(barrier, inc=1, device_id={"tm": lax.rem(me + j, peers)}, device_id_type=mesh_id)
        return 0

    lax.fori_loop(1, peers, greet, 0)
    for c in (across, right, left):
        pl.semaphore_signal(barrier, inc=1, device_id={"chan": c}, device_id_type=mesh_id)
    pl.semaphore_wait(barrier, peers + 2)

    halos = []
    for b in range(blocks):
        cp = pltpu.make_async_remote_copy(
            src_ref=source(b).at[pl.ds(0, 32)], dst_ref=x.at[b, pl.ds(256, 32)],
            send_sem=halo_send.at[b], recv_sem=halo_recv.at[b],
            device_id={"tm": before}, device_id_type=mesh_id)
        cp.start()
        halos.append(cp)

    lane = lax.broadcasted_iota(jnp.int32, (8, 128), 1)
    total = jnp.zeros((8, 128), jnp.float32)
    for b in range(blocks):
        loads[b].wait()

        def add(i, acc):
            return acc + jnp.sum(x[b, pl.ds(i * 16, 16)], axis=0)

        part = lax.fori_loop(0, 16, add, jnp.zeros((8, 128), jnp.float32))
        total = jnp.where(lane == b, jnp.sum(part, axis=1, keepdims=True), total)
    sums[0] = total

    def sum_copy(j):
        return pltpu.make_async_remote_copy(
            src_ref=sums.at[0], dst_ref=sums.at[j], send_sem=sum_send.at[j], recv_sem=sum_recv.at[j],
            device_id={"tm": lax.rem(me + j, peers)}, device_id_type=mesh_id)

    def sum_start(j, _):
        sum_copy(j).start()
        return 0

    def sum_wait(j, acc):
        sum_copy(j).wait()
        return acc + sums[j]

    lax.fori_loop(1, peers, sum_start, 0)
    total = lax.fori_loop(1, peers, sum_wait, total)
    mean = total / (256 * 128 * peers)
    for b in range(blocks):
        means[b] = jnp.broadcast_to(mean[:, b:b + 1], (8, 128))
    for b in range(blocks):
        halos[b].wait()

    x2d = x.reshape(blocks * 288 * 8, 128)
    row = lax.broadcasted_iota(jnp.int32, (64, 128), 0)
    keep = jnp.where((lax.rem(row, 8) == 7) & (me == peers - 1), 0.0, 1.0)

    def block_copy(b, j):
        slot = lax.rem(b, slots)
        to = lax.rem(me + j, peers)
        return pltpu.make_async_remote_copy(
            src_ref=send.at[slot, to], dst_ref=recv.at[b, me],
            send_sem=send_sem.at[slot, j], recv_sem=recv_sem.at[b, j],
            device_id={"tm": to}, device_id_type=mesh_id)

    def drain(b):
        def one(j, _):
            block_copy(b, j).wait_send()
            return 0
        lax.fori_loop(1, peers, one, 0)

    def landed(b):
        def one(j, _):
            block_copy(b, j).wait_recv()
            return 0
        lax.fori_loop(1, peers, one, 0)

    def piece(i, g, lo, n, c):
        return pltpu.make_async_remote_copy(
            src_ref=wv.at[g, pl.ds(lo, n)], dst_ref=wv.at[g, pl.ds(lo, n)],
            send_sem=ring_send.at[i], recv_sem=ring_recv.at[i],
            device_id={"chan": c}, device_id_type=mesh_id)

    frames = wv.shape[1]
    half = frames // 2
    zx = piece(0, mine, 0, frames, across)
    own_r = piece(1, mine, 0, frames, right)
    own_l = piece(2, mine, 0, frames, left)
    far_r = piece(3, across, 0, frames, right)
    far_l = piece(4, across, 0, frames, left)
    left_across = lax.rem(across + 6, 8)
    right_across = lax.rem(across + 2, 8)
    own_rr = piece(5, left, 0, half, right)
    own_ll = piece(6, right, half, half, left)
    far_rr = piece(7, left_across, 0, half, right)
    far_ll = piece(8, right_across, half, half, left)

    def proof_block():
        landed(0)
        gather_rows(recv.at[0], rows)
        power = []
        for w in range(8):
            r = rows[w]
            power.append(jnp.sum(r * r, axis=0, keepdims=True))
            t = flip(eye[...], r)
            mat_re[pl.ds(w, 256, stride=16), :] = t[:, :128]
            mat_re[pl.ds(8 + w, 256, stride=16), :] = t[:, 128:]

        def one(f, _):
            wv[mine, f] = mat_re[pl.ds(pl.multiple_of(f * 16, 16), 16), :].astype(jnp.bfloat16)
            return 0
        lax.fori_loop(0, 256, one, 0)
        rest = jnp.concatenate(power, axis=0)
        zero = jnp.zeros((8, 128), jnp.float32)
        for term in range(3):
            top = rest.astype(jnp.bfloat16).astype(jnp.float32)
            for h in range(2):
                wv[mine, 256 + 3 * h + term] = jnp.concatenate(
                    [top[:, 128 * h:128 * h + 128], zero], axis=0).astype(jnp.bfloat16)
            rest = rest - top
        for i in range(262, frames):
            wv[mine, i] = jnp.zeros((16, 128), jnp.bfloat16)
        zx.start()
        own_r.start()
        own_l.start()

    def aux_block(b):
        landed(b)
        gather_rows(recv.at[b], rows)
        e = eye[...]
        for c in range(8):
            r = rows[c]
            apow[b - 1, c:c + 1, :] = jnp.sum(r * r, axis=0, keepdims=True)
            t = flip(e, r)
            at = (b - 1) * 8 + c
            mat_re[pl.ds(at, 256, stride=PITCH), :] = t[:, :128]
            mat_im[pl.ds(at, 256, stride=PITCH), :] = t[:, 128:]

    def block(b, _):
        slot = lax.rem(b, slots)
        mean8 = means[b]

        def step(s, _):
            fft_step(x2d, b * 2304, mean8, scr, s, tabs)
            return 0

        lax.fori_loop(0, 8, step, 0)

        @pl.when(b >= slots)
        def _():
            drain(b - slots)

        def pack(d, _):
            for part in range(2):
                for hf in range(2):
                    at = pl.multiple_of((part * 32 + d * 2 + hf) * PITCH, 8)
                    v = scr[pl.ds(at, 64), :] * keep
                    send[slot, d, part, :, hf * 128:hf * 128 + 128] = v.astype(jnp.bfloat16)
            return 0

        lax.fori_loop(0, peers, pack, 0)

        def go(j, _):
            block_copy(b, j).start()
            return 0

        lax.fori_loop(1, peers, go, 0)
        recv[b, me] = send[slot, me]

        @pl.when(b == 1)
        def _():
            proof_block()

        @pl.when(b >= 3)
        def _():
            aux_block(b - 2)

        @pl.when(b == 4)
        def _():
            zx.wait_recv()
            far_r.start()
            far_l.start()

        @pl.when(b == 5)
        def _():
            own_r.wait_recv()
            own_l.wait_recv()
            own_rr.start()
            own_ll.start()

        @pl.when(b == 7)
        def _():
            far_r.wait_recv()
            far_l.wait_recv()
            far_rr.start()
            far_ll.start()
        return 0

    lax.fori_loop(0, blocks, block, 0)

    def store(b):
        return pltpu.make_async_copy(tile.at[lax.rem(b, 2)], num.at[pl.ds(b * 8, 8)], out_sem.at[lax.rem(b, 2)])

    def finish(b0, nb):
        n = nb * 8

        def bins(i, _):
            for u in range(8):
                f = i * 8 + u
                at = pl.ds(pl.multiple_of(f * PITCH + b0 * 8, 8), n)
                lhs = jnp.concatenate([mat_re[at, :], mat_im[at, :]], axis=0).astype(jnp.bfloat16)
                g = lax.dot_general(lhs, wv[:, f].reshape(128, 128), NT, preferred_element_type=jnp.float32)
                p, q = g[:n], g[n:]
                re = p + pltpu.roll(q, 120, 1)
                im = q - pltpu.roll(p, 120, 1)
                mat_re[at, :] = re * re + im * im
            return 0

        lax.fori_loop(0, 32, bins, 0)

        def emit(b, _):
            @pl.when(b >= 2)
            def _():
                store(b - 2).wait()
            for c in range(8):
                for h in range(2):
                    t = mat_re[pl.ds(h * 128 * PITCH + b * 8 + c, 128, stride=PITCH), :].T
                    for g in range(8):
                        tile[lax.rem(b, 2), c, 8 * g:8 * g + 8, 128 * h:128 * h + 128] = t[16 * g:16 * g + 8]
            store(b).start()
            return 0

        lax.fori_loop(b0, b0 + nb, emit, 0)

    own_rr.wait_recv()
    own_ll.wait_recv()
    far_rr.wait_recv()
    far_ll.wait_recv()
    finish(0, 4)
    aux_block(7)
    aux_block(8)
    finish(4, 4)
    for h in range(2):
        for g in range(8):
            v = [wv[g, 256 + 3 * h + term].astype(jnp.float32)[:8] for term in range(3)]
            wpow[8 * g:8 * g + 8, 128 * h:128 * h + 128] = v[0] + v[1] + v[2]
    for cp in (zx, own_r, own_l, far_r, far_l, own_rr, own_ll, far_rr, far_ll):
        cp.wait_send()
    for b in range(blocks - slots, blocks):
        drain(b)
    store(6).wait()
    store(7).wait()


def gather_rows(stage, rows):
    def one(t, _):
        for part in range(2):
            v = stage[t, part].astype(jnp.float32)
            at = pl.multiple_of(part * 128 + t * 8, 8)
            for c in range(8):
                rows[c, pl.ds(at, 8), :] = v[8 * c:8 * c + 8]
        return 0
    lax.fori_loop(0, 16, one, 0)


def flip(eye, rows_c):
    return lax.dot_general(eye, rows_c.astype(jnp.bfloat16), NT, preferred_element_type=jnp.float32)


def fused(aux, wit, peers):
    tabs = fft_tables()
    eye = jnp.eye(256, dtype=jnp.bfloat16)
    vm = pl.BlockSpec(memory_space=pltpu.VMEM)
    hbm = pl.BlockSpec(memory_space=pl.ANY)
    blocks = aux.shape[0] + 1
    slots = 3
    dma = pltpu.SemaphoreType.DMA
    f32, bf16 = jnp.float32, jnp.bfloat16
    return pl.pallas_call(
        functools.partial(fused_kernel, peers),
        out_shape=(jax.ShapeDtypeStruct((64, 64, 256), f32),
                   jax.ShapeDtypeStruct((8, 8, 256), f32),
                   jax.ShapeDtypeStruct((64, 256), f32)),
        in_specs=[hbm, hbm] + [vm] * 6,
        out_specs=(hbm, vm, vm),
        scratch_shapes=[
            pltpu.VMEM((blocks, 288, 8, 128), f32),
            pltpu.VMEM((64 * PITCH, 128), f32),
            pltpu.VMEM((slots, peers, 2, 64, 256), bf16),
            pltpu.VMEM((blocks, peers, 2, 64, 256), bf16),
            pltpu.VMEM((peers, 8, 128), f32),
            pltpu.VMEM((blocks, 8, 128), f32),
            pltpu.VMEM((8, 256, 256), f32),
            pltpu.VMEM((256 * PITCH, 128), f32),
            pltpu.VMEM((256 * PITCH, 128), f32),
            pltpu.VMEM((8, 264, 16, 128), bf16),
            pltpu.VMEM((2, 8, 64, 256), f32),
            dma((blocks,)), dma((blocks,)), dma((blocks,)),
            dma((peers,)), dma((peers,)),
            dma((slots, peers)), dma((blocks, peers)),
            dma((9,)), dma((9,)), dma((2,)),
        ],
        compiler_params=pltpu.CompilerParams(
            collective_id=0, has_side_effects=True, vmem_limit_bytes=63 * 2 ** 20),
    )(aux, wit, eye, *tabs)


def tiles(a):
    return a.reshape(a.shape[0] // 8, 8, 256, 128).transpose(0, 2, 1, 3)


def per_device(auxiliary, proofs):
    peers = lax.axis_size("tm")
    num, apow, wpow = fused(tiles(auxiliary), tiles(proofs), peers)
    apow = apow.reshape(64, 256)
    return num / ((apow[:, None, :] + 1e-06) * (wpow[None, :, :] + 1e-06))


def solution(mesh):
    return jax.shard_map(
        per_device,
        mesh=mesh,
        in_specs=(P("chan", "tm"), P("chan", "tm")),
        out_specs=P("chan", None, "tm"),
        check_vma=False,
    )
```

```python
import math
import functools
import numpy as np
import jax
import jax.numpy as jnp
from jax import lax
from jax.sharding import PartitionSpec as P
from jax.experimental import pallas as pl
from jax.experimental.pallas import tpu as pltpu

NT = (((1,), (1,)), ((), ()))
PITCH = 72


def split(x):
    hi = x.astype(jnp.bfloat16)
    lo = (x - hi.astype(jnp.float32)).astype(jnp.bfloat16)
    return hi, lo


def np_split(x):
    x = jnp.asarray(x, jnp.float32)
    return split(x)


def fft_tables():
    a = np.arange(64)
    ang = 2 * np.pi * np.outer(a, a) % (2 * np.pi * 64) / 64
    ang = 2 * np.pi * (np.outer(a, a) % 64) / 64
    f1 = np.concatenate([np.cos(ang), -np.sin(ang)], 0)
    h, l = np_split(f1)
    f1cat = jnp.concatenate([h, h, l, l], axis=1)
    lane = np.arange(128)
    k2 = np.arange(32)
    ang2 = 2 * np.pi * (np.outer(k2, lane) % 64) / 64
    re = np.concatenate([np.cos(ang2), np.sin(ang2)], 1)
    im = np.concatenate([-np.sin(ang2), np.cos(ang2)], 1)
    h, l = np_split(np.concatenate([re, im], 0))
    w2 = jnp.concatenate([h, l], axis=0)
    k1 = np.arange(128)
    angt = 2 * np.pi * (np.outer(k1, lane) % 8192) / 8192
    cos_t = jnp.asarray(np.cos(angt), jnp.float32)
    sin_t = jnp.asarray(np.sin(angt), jnp.float32)
    n = np.arange(8192)
    hann = jnp.asarray((0.5 - 0.5 * np.cos(2 * np.pi * n / 8192)).reshape(64, 128), jnp.float32)
    return f1cat, w2, cos_t, sin_t, hann


def fft_step(x2d, base, mean8, scr, s, tabs):
    f1, w2, cos_t, sin_t, hann = tabs
    cats = []
    for c in range(8):
        xs = (x2d[pl.ds(base + s * 256 + c, 64, stride=8), :] - mean8[c:c + 1]) * hann[...]
        h, l = split(xs)
        cats.append(jnp.concatenate([h, l, h, l], axis=0))
    y = jnp.dot(f1[...], jnp.concatenate(cats, axis=1), preferred_element_type=jnp.float32)
    zh, zl = [], []
    for c in range(8):
        yre = y[:64, 128 * c:128 * c + 128]
        yim = y[64:, 128 * c:128 * c + 128]
        for b in range(2):
            ct = cos_t[64 * b:64 * b + 64]
            st = sin_t[64 * b:64 * b + 64]
            h, l = split(jnp.concatenate([yre * ct + yim * st, yim * ct - yre * st], axis=1))
            zh.append(h)
            zl.append(l)
    w = w2[...]
    a = lax.dot_general(w, jnp.concatenate(zh, axis=0), NT, preferred_element_type=jnp.float32)
    b = lax.dot_general(w[:64], jnp.concatenate(zl, axis=0), NT, preferred_element_type=jnp.float32)
    o = a[:64] + a[64:] + b
    for c in range(8):
        scr[pl.ds(c * 8 + s, 64, stride=PITCH), :] = o[:, 128 * c:128 * c + 128]


def fused_kernel(peers, aux, wit, eye, f1, w2, cos_t, sin_t, hann, num, apow, wpow,
                 x, scr, send, recv, sums, means, diffs, rows, mat_re, mat_im, wv, tile,
                 load_sem, halo_send, halo_recv, sum_send, sum_recv, send_sem, recv_sem,
                 cross_send, cross_recv, ring_send, ring_recv, out_sem):
    tabs = (f1, w2, cos_t, sin_t, hann)
    mesh_id = pl.DeviceIdType.MESH
    me = lax.axis_index("tm")
    mine = lax.axis_index("chan")
    across = mine + 1 - 2 * lax.rem(mine, 2)
    right = lax.rem(mine + 2, 8)
    left = lax.rem(mine + 6, 8)
    before = lax.rem(me + peers - 1, peers)
    blocks = x.shape[0]
    slots = send.shape[0]

    def source(b):
        return wit.at[0] if b == 0 else aux.at[b - 1]

    barrier = pltpu.get_barrier_semaphore()

    def greet(j, _):
        to = lax.rem(me + j, peers)
        pl.semaphore_signal(barrier, inc=1, device_id={"tm": to}, device_id_type=mesh_id)
        pl.semaphore_signal(barrier, inc=1, device_id={"tm": to, "chan": across}, device_id_type=mesh_id)
        return 0

    lax.fori_loop(1, peers, greet, 0)
    for c in (across, right, left):
        pl.semaphore_signal(barrier, inc=1, device_id={"chan": c}, device_id_type=mesh_id)
    loads = []
    for b in range(blocks):
        cp = pltpu.make_async_copy(source(b), x.at[b, pl.ds(0, 256)], load_sem.at[b])
        cp.start()
        loads.append(cp)
    pl.semaphore_wait(barrier, 2 * (peers - 1) + 3)

    def halo(b, src):
        return pltpu.make_async_remote_copy(
            src_ref=src.at[pl.ds(0, 32)], dst_ref=x.at[b, pl.ds(256, 32)],
            send_sem=halo_send.at[b], recv_sem=halo_recv.at[b],
            device_id={"tm": before}, device_id_type=mesh_id)

    for b in range(blocks):
        halo(b, source(b)).start()

    lane = lax.broadcasted_iota(jnp.int32, (8, 128), 1)
    local = jnp.zeros((8, 128), jnp.float32)
    for b in range(blocks):
        loads[b].wait()

        def add(i, acc):
            return acc + jnp.sum(x[b, pl.ds(i * 32, 32)].reshape(8, 4, 8, 128), axis=0)

        part = jnp.sum(lax.fori_loop(0, 8, add, jnp.zeros((4, 8, 128), jnp.float32)), axis=0)
        local = jnp.where(lane == b, jnp.sum(part, axis=1, keepdims=True), local)
    sums[0] = local
    local_mean = local / (256 * 128)
    for b in range(blocks):
        means[b] = jnp.broadcast_to(local_mean[:, b:b + 1], (8, 128))

    def sum_copy(j):
        return pltpu.make_async_remote_copy(
            src_ref=sums.at[0], dst_ref=sums.at[j], send_sem=sum_send.at[j], recv_sem=sum_recv.at[j],
            device_id={"tm": lax.rem(me + j, peers)}, device_id_type=mesh_id)

    def sum_start(j, _):
        sum_copy(j).start()
        return 0

    def sum_wait(j, acc):
        sum_copy(j).wait()
        return acc + sums[j]

    lax.fori_loop(1, peers, sum_start, 0)

    def total_means():
        total = lax.fori_loop(1, peers, sum_wait, sums[0])
        mean = total / (256 * 128 * peers)
        for b in range(blocks):
            diffs[b] = means[b] - jnp.broadcast_to(mean[:, b:b + 1], (8, 128))

    x2d = x.reshape(blocks * 288 * 8, 128)
    row = lax.broadcasted_iota(jnp.int32, (64, 128), 0)
    keep = jnp.where((lax.rem(row, 8) == 7) & (me == peers - 1), 0.0, 1.0)
    col = lax.broadcasted_iota(jnp.int32, (64, 128), 1)
    hann_bins = jnp.where(col == 0, 4096.0, jnp.where(col == 1, -2048.0, 0.0))

    def block_copy(b, j):
        slot = lax.rem(b, slots)
        to = lax.rem(me + 7 * j, peers)
        return pltpu.make_async_remote_copy(
            src_ref=send.at[slot, to], dst_ref=recv.at[b, me],
            send_sem=send_sem.at[slot, j], recv_sem=recv_sem.at[b, j],
            device_id={"tm": to}, device_id_type=mesh_id)

    def drain(b):
        def one(j, _):
            block_copy(b, j).wait_send()
            return 0
        lax.fori_loop(1, peers, one, 0)

    def cross_copy(j):
        to = lax.rem(me + 7 * j, peers)
        return pltpu.make_async_remote_copy(
            src_ref=send.at[0, to], dst_ref=recv.at[blocks, me],
            send_sem=cross_send.at[j], recv_sem=cross_recv.at[j],
            device_id={"tm": to, "chan": across}, device_id_type=mesh_id)

    def landed(b):
        def one(j, _):
            block_copy(b, j).wait_recv()
            return 0
        lax.fori_loop(1, peers, one, 0)

    def piece(i, g, lo, n, c):
        return pltpu.make_async_remote_copy(
            src_ref=wv.at[g, pl.ds(lo, n)], dst_ref=wv.at[g, pl.ds(lo, n)],
            send_sem=ring_send.at[i], recv_sem=ring_recv.at[i],
            device_id={"chan": c}, device_id_type=mesh_id)

    frames = wv.shape[1]
    half = frames // 2
    left_across = lax.rem(across + 6, 8)
    right_across = lax.rem(across + 2, 8)
    own_r = piece(0, mine, 0, frames, right)
    own_l = piece(1, mine, 0, frames, left)
    far_r = piece(2, across, 0, frames, right)
    far_l = piece(3, across, 0, frames, left)
    own_rr = piece(4, left, 0, half, right)
    own_ll = piece(5, right, half, half, left)
    far_rr = piece(6, left_across, 0, half, right)
    far_ll = piece(7, right_across, half, half, left)

    def proof_piece(b, g):
        gather_rows(recv.at[b], rows)
        power = []
        for w in range(8):
            r = rows[w]
            power.append(jnp.sum(r * r, axis=0, keepdims=True))
            t = flip(eye[...], r)
            mat_re[pl.ds(w, 256, stride=16), :] = t[:, :128]
            mat_re[pl.ds(8 + w, 256, stride=16), :] = t[:, 128:]

        def one(i, _):
            for u in range(8):
                f = i * 8 + u
                wv[g, f] = mat_re[pl.ds(pl.multiple_of(f * 16, 16), 16), :].astype(jnp.bfloat16)
            return 0
        lax.fori_loop(0, 32, one, 0)
        rest = jnp.concatenate(power, axis=0)
        zero = jnp.zeros((8, 128), jnp.float32)
        for term in range(3):
            top = rest.astype(jnp.bfloat16).astype(jnp.float32)
            for h in range(2):
                wv[g, 256 + 3 * h + term] = jnp.concatenate(
                    [top[:, 128 * h:128 * h + 128], zero], axis=0).astype(jnp.bfloat16)
            rest = rest - top
        for i in range(262, frames):
            wv[g, i] = jnp.zeros((16, 128), jnp.bfloat16)

    def proof_block():
        landed(0)
        proof_piece(0, mine)
        own_r.start()
        own_l.start()

        def one(j, _):
            cross_copy(j).wait_recv()
            return 0
        lax.fori_loop(0, peers, one, 0)
        proof_piece(blocks, across)
        far_r.start()
        far_l.start()

    def aux_block(b):
        landed(b)
        gather_rows(recv.at[b], rows)
        e = eye[...]
        for c in range(8):
            r = rows[c]
            apow[b - 1, c:c + 1, :] = jnp.sum(r * r, axis=0, keepdims=True)
            t = flip(e, r)
            at = (b - 1) * 8 + c
            mat_re[pl.ds(at, 256, stride=PITCH), :] = t[:, :128]
            mat_im[pl.ds(at, 256, stride=PITCH), :] = t[:, 128:]

    def block(b, _):
        slot = lax.rem(b, slots)
        mean8 = means[b]

        def step(s, _):
            @pl.when(s == 7)
            def _():
                halo(b, aux.at[0]).wait()
            fft_step(x2d, b * 2304, mean8, scr, s, tabs)
            return 0

        lax.fori_loop(0, 8, step, 0)

        @pl.when(b == 0)
        def _():
            total_means()

        @pl.when(b >= slots)
        def _():
            drain(b - slots)

        @pl.when(b == slots)
        def _():
            def one(j, _):
                cross_copy(j).wait_send()
                return 0
            lax.fori_loop(0, peers, one, 0)

        diff = diffs[b]
        shift = jnp.concatenate([jnp.broadcast_to(diff[c:c + 1], (8, 128)) for c in range(8)], axis=0)
        scr[0:64, :] = scr[0:64, :] + shift * hann_bins

        def pack(d, _):
            for part in range(2):
                for hf in range(2):
                    at = pl.multiple_of((part * 32 + d * 2 + hf) * PITCH, 8)
                    v = scr[pl.ds(at, 64), :] * keep
                    send[slot, d, part, :, hf * 128:hf * 128 + 128] = v.astype(jnp.bfloat16)
            return 0

        lax.fori_loop(0, peers, pack, 0)

        def go(j, _):
            block_copy(b, j).start()
            return 0

        lax.fori_loop(1, peers, go, 0)
        recv[b, me] = send[slot, me]

        @pl.when(b == 0)
        def _():
            def cross(j, _):
                cross_copy(j).start()
                return 0
            lax.fori_loop(0, peers, cross, 0)

        @pl.when(b == 2)
        def _():
            proof_block()

        @pl.when(b >= 3)
        def _():
            aux_block(b - 2)

        @pl.when(b == 6)
        def _():
            own_r.wait_recv()
            own_l.wait_recv()
            own_rr.start()
            own_ll.start()

        @pl.when(b == 8)
        def _():
            far_r.wait_recv()
            far_l.wait_recv()
            far_rr.start()
            far_ll.start()
        return 0

    lax.fori_loop(0, blocks, block, 0)

    def store(b):
        return pltpu.make_async_copy(tile.at[lax.rem(b, 2)], num.at[pl.ds(b * 8, 8)], out_sem.at[lax.rem(b, 2)])

    def finish(b0, nb):
        n = nb * 8

        def bins(i, _):
            for u in range(8):
                f = i * 8 + u
                at = pl.ds(pl.multiple_of(f * PITCH + b0 * 8, 8), n)
                lhs = jnp.concatenate([mat_re[at, :], mat_im[at, :]], axis=0).astype(jnp.bfloat16)
                g = lax.dot_general(lhs, wv[:, f].reshape(128, 128), NT, preferred_element_type=jnp.float32)
                p, q = g[:n], g[n:]
                re = p + pltpu.roll(q, 120, 1)
                im = q - pltpu.roll(p, 120, 1)
                mat_re[at, :] = re * re + im * im
            return 0

        lax.fori_loop(0, 32, bins, 0)

        def emit(b, _):
            @pl.when(b >= 2)
            def _():
                store(b - 2).wait()
            for c in range(8):
                for h in range(2):
                    t = mat_re[pl.ds(h * 128 * PITCH + b * 8 + c, 128, stride=PITCH), :].T
                    for g in range(8):
                        tile[lax.rem(b, 2), c, 8 * g:8 * g + 8, 128 * h:128 * h + 128] = t[16 * g:16 * g + 8]
            store(b).start()
            return 0

        lax.fori_loop(b0, b0 + nb, emit, 0)

    aux_block(7)
    own_rr.wait_recv()
    own_ll.wait_recv()
    far_rr.wait_recv()
    far_ll.wait_recv()
    finish(0, 7)
    aux_block(8)
    finish(7, 1)
    for h in range(2):
        for g in range(8):
            v = [wv[g, 256 + 3 * h + term].astype(jnp.float32)[:8] for term in range(3)]
            wpow[8 * g:8 * g + 8, 128 * h:128 * h + 128] = v[0] + v[1] + v[2]
    for cp in (own_r, own_l, far_r, far_l, own_rr, own_ll, far_rr, far_ll):
        cp.wait_send()
    for b in range(blocks - slots, blocks):
        drain(b)
    store(6).wait()
    store(7).wait()


def gather_rows(stage, rows):
    def one(t, _):
        for part in range(2):
            v = stage[t, part].astype(jnp.float32)
            at = pl.multiple_of(part * 128 + t * 8, 8)
            for c in range(8):
                rows[c, pl.ds(at, 8), :] = v[8 * c:8 * c + 8]
        return 0
    lax.fori_loop(0, 16, one, 0)


def flip(eye, rows_c):
    return lax.dot_general(eye, rows_c.astype(jnp.bfloat16), NT, preferred_element_type=jnp.float32)


def fused(aux, wit, peers):
    tabs = fft_tables()
    eye = jnp.eye(256, dtype=jnp.bfloat16)
    vm = pl.BlockSpec(memory_space=pltpu.VMEM)
    hbm = pl.BlockSpec(memory_space=pl.ANY)
    blocks = aux.shape[0] + 1
    slots = 3
    dma = pltpu.SemaphoreType.DMA
    f32, bf16 = jnp.float32, jnp.bfloat16
    return pl.pallas_call(
        functools.partial(fused_kernel, peers),
        out_shape=(jax.ShapeDtypeStruct((64, 64, 256), f32),
                   jax.ShapeDtypeStruct((8, 8, 256), f32),
                   jax.ShapeDtypeStruct((64, 256), f32)),
        in_specs=[hbm, hbm] + [vm] * 6,
        out_specs=(hbm, vm, vm),
        scratch_shapes=[
            pltpu.VMEM((blocks, 288, 8, 128), f32),
            pltpu.VMEM((64 * PITCH, 128), f32),
            pltpu.VMEM((slots, peers, 2, 64, 256), bf16),
            pltpu.VMEM((blocks + 1, peers, 2, 64, 256), bf16),
            pltpu.VMEM((peers, 8, 128), f32),
            pltpu.VMEM((blocks, 8, 128), f32),
            pltpu.VMEM((blocks, 8, 128), f32),
            pltpu.VMEM((8, 256, 256), f32),
            pltpu.VMEM((256 * PITCH, 128), f32),
            pltpu.VMEM((256 * PITCH, 128), f32),
            pltpu.VMEM((8, 264, 16, 128), bf16),
            pltpu.VMEM((2, 8, 64, 256), f32),
            dma((blocks,)), dma((blocks,)), dma((blocks,)),
            dma((peers,)), dma((peers,)),
            dma((slots, peers)), dma((blocks, peers)),
            dma((peers,)), dma((peers,)), dma((8,)), dma((8,)), dma((2,)),
        ],
        compiler_params=pltpu.CompilerParams(
            collective_id=0, has_side_effects=True, vmem_limit_bytes=63 * 2 ** 20),
    )(aux, wit, eye, *tabs)


def tiles(a):
    return a.reshape(a.shape[0] // 8, 8, 256, 128).transpose(0, 2, 1, 3)


def per_device(auxiliary, proofs):
    peers = lax.axis_size("tm")
    num, apow, wpow = fused(tiles(auxiliary), tiles(proofs), peers)
    apow = apow.reshape(64, 256)
    return num / ((apow[:, None, :] + 1e-06) * (wpow[None, :, :] + 1e-06))


def solution(mesh):
    return jax.shard_map(
        per_device,
        mesh=mesh,
        in_specs=(P("chan", "tm"), P("chan", "tm")),
        out_specs=P("chan", None, "tm"),
        check_vma=False,
    )
```

```python
import math
import functools
import numpy as np
import jax
import jax.numpy as jnp
from jax import lax
from jax.sharding import PartitionSpec as P
from jax.experimental import pallas as pl
from jax.experimental.pallas import tpu as pltpu

NT = (((1,), (1,)), ((), ()))
PITCH = 72


def split(x):
    hi = x.astype(jnp.bfloat16)
    lo = (x - hi.astype(jnp.float32)).astype(jnp.bfloat16)
    return hi, lo


def np_split(x):
    x = jnp.asarray(x, jnp.float32)
    return split(x)


def fft_tables():
    a = np.arange(64)
    ang = 2 * np.pi * np.outer(a, a) % (2 * np.pi * 64) / 64
    ang = 2 * np.pi * (np.outer(a, a) % 64) / 64
    f1 = np.concatenate([np.cos(ang), -np.sin(ang)], 0)
    h, l = np_split(f1)
    f1cat = jnp.concatenate([h, h, l, l], axis=1)
    lane = np.arange(128)
    k2 = np.arange(32)
    ang2 = 2 * np.pi * (np.outer(k2, lane) % 64) / 64
    re = np.concatenate([np.cos(ang2), np.sin(ang2)], 1)
    im = np.concatenate([-np.sin(ang2), np.cos(ang2)], 1)
    h, l = np_split(np.concatenate([re, im], 0))
    w2 = jnp.concatenate([h, l], axis=0)
    k1 = np.arange(128)
    angt = 2 * np.pi * (np.outer(k1, lane) % 8192) / 8192
    cos_t = jnp.asarray(np.cos(angt), jnp.float32)
    sin_t = jnp.asarray(np.sin(angt), jnp.float32)
    n = np.arange(8192)
    hann = jnp.asarray((0.5 - 0.5 * np.cos(2 * np.pi * n / 8192)).reshape(64, 128), jnp.float32)
    return f1cat, w2, cos_t, sin_t, hann


def fft_step(x2d, base, mean8, scr, s, tabs):
    f1, w2, cos_t, sin_t, hann = tabs
    cats = []
    for c in range(8):
        xs = (x2d[pl.ds(base + s * 256 + c, 64, stride=8), :] - mean8[c:c + 1]) * hann[...]
        h, l = split(xs)
        cats.append(jnp.concatenate([h, l, h, l], axis=0))
    y = jnp.dot(f1[...], jnp.concatenate(cats, axis=1), preferred_element_type=jnp.float32)
    zh, zl = [], []
    for c in range(8):
        yre = y[:64, 128 * c:128 * c + 128]
        yim = y[64:, 128 * c:128 * c + 128]
        for b in range(2):
            ct = cos_t[64 * b:64 * b + 64]
            st = sin_t[64 * b:64 * b + 64]
            h, l = split(jnp.concatenate([yre * ct + yim * st, yim * ct - yre * st], axis=1))
            zh.append(h)
            zl.append(l)
    w = w2[...]
    a = lax.dot_general(w, jnp.concatenate(zh, axis=0), NT, preferred_element_type=jnp.float32)
    b = lax.dot_general(w[:64], jnp.concatenate(zl, axis=0), NT, preferred_element_type=jnp.float32)
    o = a[:64] + a[64:] + b
    for c in range(8):
        scr[pl.ds(c * 8 + s, 64, stride=PITCH), :] = o[:, 128 * c:128 * c + 128]


def fused_kernel(peers, aux, wit, f1, w2, cos_t, sin_t, hann, num, apow, wpow,
                 x, scr, send, recv, sums, means, diffs, rows, mat_re, mat_im, wv, eye,
                 load_sem, halo_send, halo_recv, sum_send, sum_recv, send_sem, recv_sem,
                 half_send, half_recv, cross_send, cross_recv, ring_send, ring_recv):
    tabs = (f1, w2, cos_t, sin_t, hann)
    mesh_id = pl.DeviceIdType.MESH
    me = lax.axis_index("tm")
    mine = lax.axis_index("chan")
    across = mine + 1 - 2 * lax.rem(mine, 2)
    right = lax.rem(mine + 2, 8)
    left = lax.rem(mine + 6, 8)
    before = lax.rem(me + peers - 1, peers)
    blocks = x.shape[0]
    slots = send.shape[0]

    def source(b):
        return wit.at[0] if b == 0 else aux.at[b - 1]

    barrier = pltpu.get_barrier_semaphore()

    def greet(j, _):
        to = lax.rem(me + j, peers)
        pl.semaphore_signal(barrier, inc=1, device_id={"tm": to}, device_id_type=mesh_id)
        pl.semaphore_signal(barrier, inc=1, device_id={"tm": to, "chan": across}, device_id_type=mesh_id)
        return 0

    lax.fori_loop(1, peers, greet, 0)
    for c in (across, right, left):
        pl.semaphore_signal(barrier, inc=1, device_id={"chan": c}, device_id_type=mesh_id)
    loads = []
    for b in range(blocks):
        cp = pltpu.make_async_copy(source(b), x.at[b, pl.ds(0, 256)], load_sem.at[b])
        cp.start()
        loads.append(cp)
    def halo(b, src):
        return pltpu.make_async_remote_copy(
            src_ref=src.at[pl.ds(0, 32)], dst_ref=x.at[b, pl.ds(256, 32)],
            send_sem=halo_send.at[b], recv_sem=halo_recv.at[b],
            device_id={"tm": before}, device_id_type=mesh_id)

    lane = lax.broadcasted_iota(jnp.int32, (8, 128), 1)

    def block_sum(b):
        def add(i, acc):
            return acc + jnp.sum(x[b, pl.ds(i * 32, 32)].reshape(8, 4, 8, 128), axis=0)

        part = jnp.sum(lax.fori_loop(0, 8, add, jnp.zeros((4, 8, 128), jnp.float32)), axis=0)
        total = jnp.sum(part, axis=1, keepdims=True)
        means[b] = jnp.broadcast_to(total / (256 * 128), (8, 128))
        return total

    def sum_copy(r, j):
        return pltpu.make_async_remote_copy(
            src_ref=sums.at[r, 0], dst_ref=sums.at[r, j],
            send_sem=sum_send.at[r, j], recv_sem=sum_recv.at[r, j],
            device_id={"tm": lax.rem(me + j, peers)}, device_id_type=mesh_id)

    def sum_start(r):
        def one(j, _):
            sum_copy(r, j).start()
            return 0
        lax.fori_loop(1, peers, one, 0)

    def total_means(r, which):
        def one(j, acc):
            sum_copy(r, j).wait()
            return acc + sums[r, j]
        total = lax.fori_loop(1, peers, one, sums[r, 0])
        mean = total / (256 * 128 * peers)
        for b in which:
            diffs[b] = means[b] - jnp.broadcast_to(mean[:, b:b + 1], (8, 128))

    loads[0].wait()
    sums[0, 0] = jnp.where(lane == 0, block_sum(0), 0.0)
    pl.semaphore_wait(barrier, 2 * (peers - 1) + 3)
    for b in range(blocks):
        halo(b, source(b)).start()
    sum_start(0)
    sums[1, 0] = jnp.zeros((8, 128), jnp.float32)
    eye[...] = (lax.broadcasted_iota(jnp.int32, (128, 128), 0)
                == lax.broadcasted_iota(jnp.int32, (128, 128), 1)).astype(jnp.float32).astype(jnp.bfloat16)

    def other_sum(b):
        pltpu.make_async_copy(aux.at[0], x.at[b, pl.ds(0, 256)], load_sem.at[b]).wait()
        sums[1, 0] = jnp.where(lane == b, block_sum(b), sums[1, 0])

    x2d = x.reshape(blocks * 288 * 8, 128)
    row = lax.broadcasted_iota(jnp.int32, (64, 128), 0)
    keep = jnp.where((lax.rem(row, 8) == 7) & (me == peers - 1), 0.0, 1.0)
    col = lax.broadcasted_iota(jnp.int32, (64, 128), 1)
    hann_bins = jnp.where(col == 0, 4096.0, jnp.where(col == 1, -2048.0, 0.0))

    def block_copy(b, j):
        slot = lax.rem(b, slots)
        to = lax.rem(me + 7 * j, peers)
        return pltpu.make_async_remote_copy(
            src_ref=send.at[slot, to], dst_ref=recv.at[b, me],
            send_sem=send_sem.at[slot, j], recv_sem=recv_sem.at[b, j],
            device_id={"tm": to}, device_id_type=mesh_id)

    def drain(b):
        def one(j, _):
            block_copy(b, j).wait_send()
            return 0
        lax.fori_loop(1, peers, one, 0)

    def half_copy(hf, j):
        to = lax.rem(me + 7 * j, peers)
        return pltpu.make_async_remote_copy(
            src_ref=send.at[(blocks - 1) % slots, to, hf], dst_ref=recv.at[blocks - 1, me, hf],
            send_sem=half_send.at[hf, j], recv_sem=half_recv.at[hf, j],
            device_id={"tm": to}, device_id_type=mesh_id)

    def half_wait(hf, send_side):
        def one(j, _):
            if send_side:
                half_copy(hf, j).wait_send()
            else:
                half_copy(hf, j).wait_recv()
            return 0
        lax.fori_loop(1, peers, one, 0)

    def cross_copy(j):
        to = lax.rem(me + 7 * j, peers)
        return pltpu.make_async_remote_copy(
            src_ref=send.at[0, to], dst_ref=recv.at[blocks, me],
            send_sem=cross_send.at[j], recv_sem=cross_recv.at[j],
            device_id={"tm": to, "chan": across}, device_id_type=mesh_id)

    def landed(b):
        def one(j, _):
            block_copy(b, j).wait_recv()
            return 0
        lax.fori_loop(1, peers, one, 0)

    def piece(i, g, lo, n, c):
        return pltpu.make_async_remote_copy(
            src_ref=wv.at[g, pl.ds(lo, n)], dst_ref=wv.at[g, pl.ds(lo, n)],
            send_sem=ring_send.at[i], recv_sem=ring_recv.at[i],
            device_id={"chan": c}, device_id_type=mesh_id)

    frames = wv.shape[1]
    half = frames // 2
    left_across = lax.rem(across + 6, 8)
    right_across = lax.rem(across + 2, 8)
    own_r = piece(0, mine, 0, frames, right)
    own_l = piece(1, mine, 0, frames, left)
    far_r = piece(2, across, 0, frames, right)
    far_l = piece(3, across, 0, frames, left)
    own_rr = piece(4, left, 0, half, right)
    own_ll = piece(5, right, half, half, left)
    far_rr = piece(6, left_across, 0, half, right)
    far_ll = piece(7, right_across, half, half, left)

    def proof_piece(b, g):
        power = []
        for h in range(2):
            gather_rows(recv.at[b], rows, h)
            for w in range(8):
                r = rows[w]
                power.append(jnp.sum(r * r, axis=0, keepdims=True))
                t = flip(eye[...], r)
                mat_re[pl.ds(h * 2048 + w, 128, stride=16), :] = t[:, :128]
                mat_re[pl.ds(h * 2048 + 8 + w, 128, stride=16), :] = t[:, 128:]

        def one(i, _):
            for u in range(8):
                f = i * 8 + u
                wv[g, f] = mat_re[pl.ds(pl.multiple_of(f * 16, 16), 16), :].astype(jnp.bfloat16)
            return 0
        lax.fori_loop(0, 32, one, 0)
        zero = jnp.zeros((8, 128), jnp.float32)
        for h in range(2):
            rest = jnp.concatenate(power[8 * h:8 * h + 8], axis=0)
            for term in range(3):
                top = rest.astype(jnp.bfloat16).astype(jnp.float32)
                wv[g, 256 + 3 * h + term] = jnp.concatenate([top, zero], axis=0).astype(jnp.bfloat16)
                rest = rest - top
        for i in range(262, frames):
            wv[g, i] = jnp.zeros((16, 128), jnp.bfloat16)

    def proof_own():
        landed(0)
        proof_piece(0, mine)
        own_r.start()
        own_l.start()

    def proof_across():
        def one(j, _):
            cross_copy(j).wait_recv()
            return 0
        lax.fori_loop(0, peers, one, 0)
        proof_piece(blocks, across)
        far_r.start()
        far_l.start()

    def aux_half(b, h):
        gather_rows(recv.at[b], rows, h)
        e = eye[...]
        for c in range(8):
            r = rows[c]
            apow[b - 1, c:c + 1, 128 * h:128 * h + 128] = jnp.sum(r * r, axis=0, keepdims=True)
            t = flip(e, r)
            at = h * 128 * PITCH + (b - 1) * 8 + c
            mat_re[pl.ds(at, 128, stride=PITCH), :] = t[:, :128]
            mat_im[pl.ds(at, 128, stride=PITCH), :] = t[:, 128:]

    def aux_block(b):
        landed(b)
        aux_half(b, 0)
        aux_half(b, 1)

    def block(b, _):
        slot = lax.rem(b, slots)
        mean8 = means[b]

        def step(s, _):
            @pl.when(s == 7)
            def _():
                halo(b, aux.at[0]).wait()
            fft_step(x2d, b * 2304, mean8, scr, s, tabs)

            @pl.when(b == 0)
            def _():
                other_sum(s + 1)
            return 0

        lax.fori_loop(0, 8, step, 0)

        @pl.when(b == 0)
        def _():
            sum_start(1)
            total_means(0, range(1))

        @pl.when(b == 1)
        def _():
            total_means(1, range(1, blocks))

        @pl.when(b >= slots)
        def _():
            drain(b - slots)

        @pl.when(b == slots)
        def _():
            def one(j, _):
                cross_copy(j).wait_send()
                return 0
            lax.fori_loop(0, peers, one, 0)

        diff = diffs[b]
        shift = jnp.concatenate([jnp.broadcast_to(diff[c:c + 1], (8, 128)) for c in range(8)], axis=0)
        scr[0:64, :] = scr[0:64, :] + shift * hann_bins

        def pack(d, _):
            for part in range(2):
                for hf in range(2):
                    at = pl.multiple_of((part * 32 + d * 2 + hf) * PITCH, 8)
                    v = scr[pl.ds(at, 64), :] * keep
                    send[slot, d, hf, part] = v.astype(jnp.bfloat16)
            return 0

        lax.fori_loop(0, peers, pack, 0)

        @pl.when(b < blocks - 1)
        def _():
            def go(j, _):
                block_copy(b, j).start()
                return 0
            lax.fori_loop(1, peers, go, 0)

        @pl.when(b == blocks - 1)
        def _():
            for hf in range(2):
                def go(j, _):
                    half_copy(hf, j).start()
                    return 0
                lax.fori_loop(1, peers, go, 0)

        recv[b, me] = send[slot, me]

        @pl.when(b == 0)
        def _():
            def cross(j, _):
                cross_copy(j).start()
                return 0
            lax.fori_loop(0, peers, cross, 0)

        @pl.when(b == 1)
        def _():
            proof_own()

        @pl.when(b == 2)
        def _():
            proof_across()

        @pl.when(b >= 3)
        def _():
            aux_block(b - 2)

        @pl.when(b == 5)
        def _():
            own_r.wait_recv()
            own_l.wait_recv()
            own_rr.start()
            own_ll.start()

        @pl.when(b == 7)
        def _():
            far_r.wait_recv()
            far_l.wait_recv()
            far_rr.start()
            far_ll.start()
        return 0

    lax.fori_loop(0, blocks, block, 0)

    def finish(b0, nb, h):
        n = nb * 8

        def bins(i, _):
            got = []
            for u in range(32):
                f = h * 128 + i * 32 + u
                at = pl.ds(pl.multiple_of(f * PITCH + b0 * 8, 8), n)
                lhs = jnp.concatenate([mat_re[at, :], mat_im[at, :]], axis=0).astype(jnp.bfloat16)
                g = lax.dot_general(lhs, wv[:, f].reshape(128, 128), NT, preferred_element_type=jnp.float32)
                p, q = g[:n], g[n:]
                re = p + pltpu.roll(q, 120, 1)
                im = q - pltpu.roll(p, 120, 1)
                mat_re[at, :] = re * re + im * im
            return 0

        lax.fori_loop(0, 4, bins, 0)

        def emit(b, _):
            for c in range(8):
                t = mat_re[pl.ds(h * 128 * PITCH + b * 8 + c, 128, stride=PITCH), :].T
                for g in range(8):
                    num[b * 8 + c, 8 * g:8 * g + 8, 128 * h:128 * h + 128] = t[16 * g:16 * g + 8]
            return 0

        lax.fori_loop(b0, b0 + nb, emit, 0)

    own_rr.wait_recv()
    own_ll.wait_recv()
    far_rr.wait_recv()
    far_ll.wait_recv()
    for h in range(2):
        for g in range(8):
            v = [wv[g, 256 + 3 * h + term].astype(jnp.float32)[:8] for term in range(3)]
            wpow[8 * g:8 * g + 8, 128 * h:128 * h + 128] = v[0] + v[1] + v[2]
    early = blocks - 3
    for h in range(2):
        finish(0, early, h)
    aux_block(blocks - 2)
    for h in range(2):
        half_wait(h, False)
        aux_half(blocks - 1, h)
        finish(early, 2, h)
    for cp in (own_r, own_l, far_r, far_l, own_rr, own_ll, far_rr, far_ll):
        cp.wait_send()
    for b in range(blocks - slots, blocks - 1):
        drain(b)
    for h in range(2):
        half_wait(h, True)


def gather_rows(stage, rows, h):
    def one(t, _):
        for part in range(2):
            v = stage[t, h, part].astype(jnp.float32)
            at = pl.multiple_of(part * 128 + t * 8, 8)
            for c in range(8):
                rows[c, pl.ds(at, 8), :] = v[8 * c:8 * c + 8]
        return 0
    lax.fori_loop(0, 16, one, 0)


def flip(eye, rows_c):
    return lax.dot_general(eye, rows_c.astype(jnp.bfloat16), NT, preferred_element_type=jnp.float32)


def fused(aux, wit, peers):
    tabs = fft_tables()
    vm = pl.BlockSpec(memory_space=pltpu.VMEM)
    hbm = pl.BlockSpec(memory_space=pl.ANY)
    blocks = aux.shape[0] + 1
    slots = 3
    dma = pltpu.SemaphoreType.DMA
    f32, bf16 = jnp.float32, jnp.bfloat16
    return pl.pallas_call(
        functools.partial(fused_kernel, peers),
        out_shape=(jax.ShapeDtypeStruct((64, 64, 256), f32),
                   jax.ShapeDtypeStruct((8, 8, 256), f32),
                   jax.ShapeDtypeStruct((64, 256), f32)),
        in_specs=[hbm, hbm] + [vm] * 5,
        out_specs=(vm, vm, vm),
        scratch_shapes=[
            pltpu.VMEM((blocks, 288, 8, 128), f32),
            pltpu.VMEM((64 * PITCH, 128), f32),
            pltpu.VMEM((slots, peers, 2, 2, 64, 128), bf16),
            pltpu.VMEM((blocks + 1, peers, 2, 2, 64, 128), bf16),
            pltpu.VMEM((2, peers, 8, 128), f32),
            pltpu.VMEM((blocks, 8, 128), f32),
            pltpu.VMEM((blocks, 8, 128), f32),
            pltpu.VMEM((8, 256, 128), f32),
            pltpu.VMEM((256 * PITCH, 128), f32),
            pltpu.VMEM((256 * PITCH, 128), f32),
            pltpu.VMEM((8, 264, 16, 128), bf16),
            pltpu.VMEM((128, 128), bf16),
            dma((blocks,)), dma((blocks,)), dma((blocks,)),
            dma((2, peers)), dma((2, peers)),
            dma((slots, peers)), dma((blocks, peers)),
            dma((2, peers)), dma((2, peers)),
            dma((peers,)), dma((peers,)), dma((8,)), dma((8,)),
        ],
        compiler_params=pltpu.CompilerParams(
            collective_id=0, has_side_effects=True, vmem_limit_bytes=63 * 2 ** 20),
    )(aux, wit, *tabs)


def tiles(a):
    return a.reshape(a.shape[0] // 8, 8, 256, 128).transpose(0, 2, 1, 3)


def per_device(auxiliary, proofs):
    peers = lax.axis_size("tm")
    num, apow, wpow = fused(tiles(auxiliary), tiles(proofs), peers)
    apow = apow.reshape(64, 256)
    return num / ((apow[:, None, :] + 1e-06) * (wpow[None, :, :] + 1e-06))


def solution(mesh):
    return jax.shard_map(
        per_device,
        mesh=mesh,
        in_specs=(P("chan", "tm"), P("chan", "tm")),
        out_specs=P("chan", None, "tm"),
        check_vma=False,
    )
```

```python
import math
import functools
import numpy as np
import jax
import jax.numpy as jnp
from jax import lax
from jax.sharding import PartitionSpec as P
from jax.experimental import pallas as pl
from jax.experimental.pallas import tpu as pltpu

NT = (((1,), (1,)), ((), ()))
PITCH = 72


def split(x):
    hi = x.astype(jnp.bfloat16)
    lo = (x - hi.astype(jnp.float32)).astype(jnp.bfloat16)
    return hi, lo


def np_split(x):
    x = jnp.asarray(x, jnp.float32)
    return split(x)


def fft_tables():
    a = np.arange(64)
    ang = 2 * np.pi * np.outer(a, a) % (2 * np.pi * 64) / 64
    ang = 2 * np.pi * (np.outer(a, a) % 64) / 64
    f1 = np.concatenate([np.cos(ang), -np.sin(ang)], 0)
    h, l = np_split(f1)
    f1cat = jnp.concatenate([h, h, l, l], axis=1)
    lane = np.arange(128)
    k2 = np.arange(32)
    ang2 = 2 * np.pi * (np.outer(k2, lane) % 64) / 64
    re = np.concatenate([np.cos(ang2), np.sin(ang2)], 1)
    im = np.concatenate([-np.sin(ang2), np.cos(ang2)], 1)
    h, l = np_split(np.concatenate([re, im], 0))
    w2 = jnp.concatenate([h, l], axis=0)
    k1 = np.arange(128)
    angt = 2 * np.pi * (np.outer(k1, lane) % 8192) / 8192
    cos_t = jnp.asarray(np.cos(angt), jnp.float32)
    sin_t = jnp.asarray(np.sin(angt), jnp.float32)
    n = np.arange(8192)
    hann = jnp.asarray((0.5 - 0.5 * np.cos(2 * np.pi * n / 8192)).reshape(64, 128), jnp.float32)
    return f1cat, w2, cos_t, sin_t, hann


def fft_step(x2d, base, mean8, scr, s, tabs):
    f1, w2, cos_t, sin_t, hann = tabs
    cats = []
    for c in range(8):
        xs = (x2d[pl.ds(base + s * 256 + c, 64, stride=8), :] - mean8[c:c + 1]) * hann[...]
        h, l = split(xs)
        cats.append(jnp.concatenate([h, l, h, l], axis=0))
    y = jnp.dot(f1[...], jnp.concatenate(cats, axis=1), preferred_element_type=jnp.float32)
    zh, zl = [], []
    for c in range(8):
        yre = y[:64, 128 * c:128 * c + 128]
        yim = y[64:, 128 * c:128 * c + 128]
        for b in range(2):
            ct = cos_t[64 * b:64 * b + 64]
            st = sin_t[64 * b:64 * b + 64]
            h, l = split(jnp.concatenate([yre * ct + yim * st, yim * ct - yre * st], axis=1))
            zh.append(h)
            zl.append(l)
    w = w2[...]
    a = lax.dot_general(w, jnp.concatenate(zh, axis=0), NT, preferred_element_type=jnp.float32)
    b = lax.dot_general(w[:64], jnp.concatenate(zl, axis=0), NT, preferred_element_type=jnp.float32)
    o = a[:64] + a[64:] + b
    for c in range(8):
        scr[pl.ds(c * 8 + s, 64, stride=PITCH), :] = o[:, 128 * c:128 * c + 128]


def fused_kernel(peers, aux, wit, f1, w2, cos_t, sin_t, hann, num, apow, wpow,
                 x, scr, send, recv, sums, means, diffs, rows, mat_re, mat_im, wv, eye, ybuf, numv,
                 load_sem, halo_send, halo_recv, sum_send, sum_recv, send_sem, recv_sem,
                 half_send, half_recv, y_send, y_recv, z_send, z_recv, ring_send, ring_recv, out_sem):
    tabs = (f1, w2, cos_t, sin_t, hann)
    mesh_id = pl.DeviceIdType.MESH
    me = lax.axis_index("tm")
    mine = lax.axis_index("chan")
    across = mine + 1 - 2 * lax.rem(mine, 2)
    right = lax.rem(mine + 2, 8)
    left = lax.rem(mine + 6, 8)
    before = lax.rem(me + peers - 1, peers)
    ring = peers // 2
    spot = lax.rem(me, ring)
    side = (me - spot) // ring
    facing = (1 - side) * ring + spot
    blocks = x.shape[0]
    slots = send.shape[0]

    def source(b):
        return wit.at[0] if b == 0 else aux.at[b - 1]

    barrier = pltpu.get_barrier_semaphore()

    def greet(j, _):
        to = lax.rem(me + j, peers)
        pl.semaphore_signal(barrier, inc=1, device_id={"tm": to}, device_id_type=mesh_id)
        return 0

    lax.fori_loop(1, peers, greet, 0)
    pl.semaphore_signal(barrier, inc=1, device_id={"tm": facing, "chan": across}, device_id_type=mesh_id)
    for c in (across, right, left):
        pl.semaphore_signal(barrier, inc=1, device_id={"chan": c}, device_id_type=mesh_id)
    loads = []
    for b in range(blocks):
        cp = pltpu.make_async_copy(source(b), x.at[b, pl.ds(0, 256)], load_sem.at[b])
        cp.start()
        loads.append(cp)
    def halo(b, src):
        return pltpu.make_async_remote_copy(
            src_ref=src.at[pl.ds(0, 32)], dst_ref=x.at[b, pl.ds(256, 32)],
            send_sem=halo_send.at[b], recv_sem=halo_recv.at[b],
            device_id={"tm": before}, device_id_type=mesh_id)

    lane = lax.broadcasted_iota(jnp.int32, (8, 128), 1)

    def block_sum(b):
        def add(i, acc):
            return acc + jnp.sum(x[b, pl.ds(i * 32, 32)].reshape(8, 4, 8, 128), axis=0)

        part = jnp.sum(lax.fori_loop(0, 8, add, jnp.zeros((4, 8, 128), jnp.float32)), axis=0)
        total = jnp.sum(part, axis=1, keepdims=True)
        means[b] = jnp.broadcast_to(total / (256 * 128), (8, 128))
        return total

    def sum_copy(r, j):
        return pltpu.make_async_remote_copy(
            src_ref=sums.at[r, 0], dst_ref=sums.at[r, j],
            send_sem=sum_send.at[r, j], recv_sem=sum_recv.at[r, j],
            device_id={"tm": lax.rem(me + j, peers)}, device_id_type=mesh_id)

    def sum_start(r):
        def one(j, _):
            sum_copy(r, j).start()
            return 0
        lax.fori_loop(1, peers, one, 0)

    def total_means(r, which):
        def one(j, acc):
            sum_copy(r, j).wait()
            return acc + sums[r, j]
        total = lax.fori_loop(1, peers, one, sums[r, 0])
        mean = total / (256 * 128 * peers)
        for b in which:
            diffs[b] = means[b] - jnp.broadcast_to(mean[:, b:b + 1], (8, 128))

    loads[0].wait()
    sums[0, 0] = jnp.where(lane == 0, block_sum(0), 0.0)
    pl.semaphore_wait(barrier, peers - 1 + 4)
    for b in range(blocks):
        halo(b, source(b)).start()
    sum_start(0)
    sums[1, 0] = jnp.zeros((8, 128), jnp.float32)
    eye[...] = (lax.broadcasted_iota(jnp.int32, (128, 128), 0)
                == lax.broadcasted_iota(jnp.int32, (128, 128), 1)).astype(jnp.float32).astype(jnp.bfloat16)

    def other_sum(b):
        pltpu.make_async_copy(aux.at[0], x.at[b, pl.ds(0, 256)], load_sem.at[b]).wait()
        sums[1, 0] = jnp.where(lane == b, block_sum(b), sums[1, 0])

    x2d = x.reshape(blocks * 288 * 8, 128)
    row = lax.broadcasted_iota(jnp.int32, (64, 128), 0)
    keep = jnp.where((lax.rem(row, 8) == 7) & (me == peers - 1), 0.0, 1.0)
    col = lax.broadcasted_iota(jnp.int32, (64, 128), 1)
    hann_bins = jnp.where(col == 0, 4096.0, jnp.where(col == 1, -2048.0, 0.0))

    def block_copy(b, j):
        slot = lax.rem(b, slots)
        to = lax.rem(me + 7 * j, peers)
        return pltpu.make_async_remote_copy(
            src_ref=send.at[slot, to], dst_ref=recv.at[b, me],
            send_sem=send_sem.at[slot, j], recv_sem=recv_sem.at[b, j],
            device_id={"tm": to}, device_id_type=mesh_id)

    def drain(b):
        def one(j, _):
            block_copy(b, j).wait_send()
            return 0
        lax.fori_loop(1, peers, one, 0)

    def half_copy(hf, j):
        to = lax.rem(me + 7 * j, peers)
        return pltpu.make_async_remote_copy(
            src_ref=send.at[(blocks - 1) % slots, to, hf], dst_ref=recv.at[blocks - 1, me, hf],
            send_sem=half_send.at[hf, j], recv_sem=half_recv.at[hf, j],
            device_id={"tm": to}, device_id_type=mesh_id)

    def half_wait(hf, send_side):
        def one(j, _):
            if send_side:
                half_copy(hf, j).wait_send()
            else:
                half_copy(hf, j).wait_recv()
            return 0
        lax.fori_loop(1, peers, one, 0)

    def y_copy(k, j):
        to = lax.rem(spot + 3 * j, ring)
        return pltpu.make_async_remote_copy(
            src_ref=send.at[0, k * ring + to], dst_ref=ybuf.at[k, spot],
            send_sem=y_send.at[k, j], recv_sem=y_recv.at[k, j],
            device_id={"tm": side * ring + to}, device_id_type=mesh_id)

    def y_each(act):
        def one(j, _):
            for k in range(2):
                act(y_copy(k, j))
            return 0
        lax.fori_loop(1, ring, one, 0)

    def z_copy(i, k, b, dev):
        return pltpu.make_async_remote_copy(
            src_ref=ybuf.at[k], dst_ref=recv.at[b, pl.ds(side * ring, ring)],
            send_sem=z_send.at[i], recv_sem=z_recv.at[i],
            device_id=dev, device_id_type=mesh_id)

    z_copies = [z_copy(0, 1 - side, 0, {"tm": facing}),
                z_copy(1, 1 - side, blocks, {"tm": facing, "chan": across}),
                z_copy(2, side, blocks, {"chan": across})]

    def z_phase():
        y_each(lambda cp: cp.wait_recv())
        for cp in z_copies:
            cp.start()
        for i in range(ring):
            recv[0, side * ring + i] = ybuf[side, i]

    def landed(b):
        def one(j, _):
            block_copy(b, j).wait_recv()
            return 0
        lax.fori_loop(1, peers, one, 0)

    def piece(i, g, lo, n, c):
        return pltpu.make_async_remote_copy(
            src_ref=wv.at[g, pl.ds(lo, n)], dst_ref=wv.at[g, pl.ds(lo, n)],
            send_sem=ring_send.at[i], recv_sem=ring_recv.at[i],
            device_id={"chan": c}, device_id_type=mesh_id)

    frames = wv.shape[1]
    half = frames // 2
    left_across = lax.rem(across + 6, 8)
    right_across = lax.rem(across + 2, 8)
    own_r = piece(0, mine, 0, frames, right)
    own_l = piece(1, mine, 0, frames, left)
    far_r = piece(2, across, 0, frames, right)
    far_l = piece(3, across, 0, frames, left)
    own_rr = piece(4, left, 0, half, right)
    own_ll = piece(5, right, half, half, left)
    far_rr = piece(6, left_across, 0, half, right)
    far_ll = piece(7, right_across, half, half, left)

    def proof_piece(b, g):
        power = []
        for h in range(2):
            gather_rows(recv.at[b], rows, h)
            for w in range(8):
                r = rows[w]
                power.append(jnp.sum(r * r, axis=0, keepdims=True))
                t = flip(eye[...], r)
                mat_re[pl.ds(h * 2048 + w, 128, stride=16), :] = t[:, :128]
                mat_re[pl.ds(h * 2048 + 8 + w, 128, stride=16), :] = t[:, 128:]

        def one(i, _):
            for u in range(8):
                f = i * 8 + u
                wv[g, f] = mat_re[pl.ds(pl.multiple_of(f * 16, 16), 16), :].astype(jnp.bfloat16)
            return 0
        lax.fori_loop(0, 32, one, 0)
        zero = jnp.zeros((8, 128), jnp.float32)
        for h in range(2):
            rest = jnp.concatenate(power[8 * h:8 * h + 8], axis=0)
            for term in range(3):
                top = rest.astype(jnp.bfloat16).astype(jnp.float32)
                wv[g, 256 + 3 * h + term] = jnp.concatenate([top, zero], axis=0).astype(jnp.bfloat16)
                rest = rest - top
        for i in range(262, frames):
            wv[g, i] = jnp.zeros((16, 128), jnp.bfloat16)

    def proof_own():
        z_copies[0].wait_recv()
        proof_piece(0, mine)
        own_r.start()
        own_l.start()

    def proof_across():
        z_copies[1].wait_recv()
        z_copies[2].wait_recv()
        proof_piece(blocks, across)
        far_r.start()
        far_l.start()

    def aux_half(b, h):
        gather_rows(recv.at[b], rows, h)
        e = eye[...]
        for c in range(8):
            r = rows[c]
            apow[b - 1, c:c + 1, 128 * h:128 * h + 128] = jnp.sum(r * r, axis=0, keepdims=True)
            t = flip(e, r)
            at = h * 128 * PITCH + (b - 1) * 8 + c
            mat_re[pl.ds(at, 128, stride=PITCH), :] = t[:, :128]
            mat_im[pl.ds(at, 128, stride=PITCH), :] = t[:, 128:]

    def aux_block(b):
        landed(b)
        aux_half(b, 0)
        aux_half(b, 1)

    def block(b, _):
        slot = lax.rem(b, slots)
        mean8 = means[b]

        def step(s, _):
            @pl.when(s == 7)
            def _():
                halo(b, aux.at[0]).wait()
            fft_step(x2d, b * 2304, mean8, scr, s, tabs)

            @pl.when(b == 0)
            def _():
                other_sum(s + 1)
            return 0

        lax.fori_loop(0, 8, step, 0)

        @pl.when(b == 0)
        def _():
            sum_start(1)
            total_means(0, range(1))

        @pl.when(b == 1)
        def _():
            total_means(1, range(1, blocks))
            z_phase()

        @pl.when(b > slots)
        def _():
            drain(b - slots)

        @pl.when(b == slots)
        def _():
            y_each(lambda cp: cp.wait_send())

        diff = diffs[b]
        shift = jnp.concatenate([jnp.broadcast_to(diff[c:c + 1], (8, 128)) for c in range(8)], axis=0)
        scr[0:64, :] = scr[0:64, :] + shift * hann_bins

        def pack(d, _):
            for part in range(2):
                for hf in range(2):
                    at = pl.multiple_of((part * 32 + d * 2 + hf) * PITCH, 8)
                    v = scr[pl.ds(at, 64), :] * keep
                    send[slot, d, hf, part] = v.astype(jnp.bfloat16)
            return 0

        lax.fori_loop(0, peers, pack, 0)

        @pl.when(b == 0)
        def _():
            y_each(lambda cp: cp.start())
            for k in range(2):
                ybuf[k, spot] = send[0, k * ring + spot]

        @pl.when((b > 0) & (b < blocks - 1))
        def _():
            def go(j, _):
                block_copy(b, j).start()
                return 0
            lax.fori_loop(1, peers, go, 0)

        @pl.when(b == blocks - 1)
        def _():
            for hf in range(2):
                def go(j, _):
                    half_copy(hf, j).start()
                    return 0
                lax.fori_loop(1, peers, go, 0)

        @pl.when(b > 0)
        def _():
            recv[b, me] = send[slot, me]

        @pl.when(b == 2)
        def _():
            proof_own()

        @pl.when(b == 3)
        def _():
            proof_across()

        @pl.when(b >= 3)
        def _():
            aux_block(b - 2)

        @pl.when(b == 5)
        def _():
            own_r.wait_recv()
            own_l.wait_recv()
            own_rr.start()
            own_ll.start()

        @pl.when(b == 8)
        def _():
            far_r.wait_recv()
            far_l.wait_recv()
            far_rr.start()
            far_ll.start()
        return 0

    lax.fori_loop(0, blocks, block, 0)

    def finish(b0, nb, h):
        n = nb * 8

        def bins(i, _):
            got = []
            for u in range(32):
                f = h * 128 + i * 32 + u
                at = pl.ds(pl.multiple_of(f * PITCH + b0 * 8, 8), n)
                lhs = jnp.concatenate([mat_re[at, :], mat_im[at, :]], axis=0).astype(jnp.bfloat16)
                g = lax.dot_general(lhs, wv[:, f].reshape(128, 128), NT, preferred_element_type=jnp.float32)
                p, q = g[:n], g[n:]
                re = p + pltpu.roll(q, 120, 1)
                im = q - pltpu.roll(p, 120, 1)
                mat_re[at, :] = re * re + im * im
            return 0

        lax.fori_loop(0, 4, bins, 0)

        def emit(b, _):
            for c in range(8):
                t = mat_re[pl.ds(h * 128 * PITCH + b * 8 + c, 128, stride=PITCH), :].T
                for g in range(8):
                    numv[b * 8 + c, 8 * g:8 * g + 8, 128 * h:128 * h + 128] = t[16 * g:16 * g + 8]
            return 0

        lax.fori_loop(b0, b0 + nb, emit, 0)

    own_rr.wait_recv()
    own_ll.wait_recv()
    far_rr.wait_recv()
    far_ll.wait_recv()
    for h in range(2):
        for g in range(8):
            v = [wv[g, 256 + 3 * h + term].astype(jnp.float32)[:8] for term in range(3)]
            wpow[8 * g:8 * g + 8, 128 * h:128 * h + 128] = v[0] + v[1] + v[2]
    early = blocks - 3
    for h in range(2):
        finish(0, early, h)

    def out_copy(i, b, n):
        return pltpu.make_async_copy(numv.at[pl.ds(8 * b, 8 * n)], num.at[pl.ds(8 * b, 8 * n)], out_sem.at[i])

    out_copy(0, 0, early).start()
    aux_block(blocks - 2)
    for h in range(2):
        half_wait(h, False)
        aux_half(blocks - 1, h)
        finish(early, 2, h)
    out_copy(1, early, 2).start()
    for cp in (own_r, own_l, far_r, far_l, own_rr, own_ll, far_rr, far_ll):
        cp.wait_send()
    for b in range(blocks - slots, blocks - 1):
        drain(b)
    for h in range(2):
        half_wait(h, True)
    for cp in z_copies:
        cp.wait_send()
    out_copy(0, 0, early).wait()
    out_copy(1, early, 2).wait()


def gather_rows(stage, rows, h):
    def one(t, _):
        for part in range(2):
            v = stage[t, h, part].astype(jnp.float32)
            at = pl.multiple_of(part * 128 + t * 8, 8)
            for c in range(8):
                rows[c, pl.ds(at, 8), :] = v[8 * c:8 * c + 8]
        return 0
    lax.fori_loop(0, 16, one, 0)


def flip(eye, rows_c):
    return lax.dot_general(eye, rows_c.astype(jnp.bfloat16), NT, preferred_element_type=jnp.float32)


def fused(aux, wit, peers):
    tabs = fft_tables()
    vm = pl.BlockSpec(memory_space=pltpu.VMEM)
    hbm = pl.BlockSpec(memory_space=pl.ANY)
    blocks = aux.shape[0] + 1
    slots = 3
    dma = pltpu.SemaphoreType.DMA
    f32, bf16 = jnp.float32, jnp.bfloat16
    return pl.pallas_call(
        functools.partial(fused_kernel, peers),
        out_shape=(jax.ShapeDtypeStruct((64, 64, 256), f32),
                   jax.ShapeDtypeStruct((8, 8, 256), f32),
                   jax.ShapeDtypeStruct((64, 256), f32)),
        in_specs=[hbm, hbm] + [vm] * 5,
        out_specs=(hbm, vm, vm),
        scratch_shapes=[
            pltpu.VMEM((blocks, 288, 8, 128), f32),
            pltpu.VMEM((64 * PITCH, 128), f32),
            pltpu.VMEM((slots, peers, 2, 2, 64, 128), bf16),
            pltpu.VMEM((blocks + 1, peers, 2, 2, 64, 128), bf16),
            pltpu.VMEM((2, peers, 8, 128), f32),
            pltpu.VMEM((blocks, 8, 128), f32),
            pltpu.VMEM((blocks, 8, 128), f32),
            pltpu.VMEM((8, 256, 128), f32),
            pltpu.VMEM((256 * PITCH, 128), f32),
            pltpu.VMEM((256 * PITCH, 128), f32),
            pltpu.VMEM((8, 264, 16, 128), bf16),
            pltpu.VMEM((128, 128), bf16),
            pltpu.VMEM((2, peers // 2, 2, 2, 64, 128), bf16),
            pltpu.VMEM((64, 64, 256), f32),
            dma((blocks,)), dma((blocks,)), dma((blocks,)),
            dma((2, peers)), dma((2, peers)),
            dma((slots, peers)), dma((blocks, peers)),
            dma((2, peers)), dma((2, peers)),
            dma((2, peers // 2)), dma((2, peers // 2)), dma((3,)), dma((3,)),
            dma((8,)), dma((8,)), dma((2,)),
        ],
        compiler_params=pltpu.CompilerParams(
            collective_id=0, has_side_effects=True, vmem_limit_bytes=63 * 2 ** 20),
    )(aux, wit, *tabs)


def tiles(a):
    return a.reshape(a.shape[0] // 8, 8, 256, 128).transpose(0, 2, 1, 3)


def per_device(auxiliary, proofs):
    peers = lax.axis_size("tm")
    num, apow, wpow = fused(tiles(auxiliary), tiles(proofs), peers)
    apow = apow.reshape(64, 256)
    return num / ((apow[:, None, :] + 1e-06) * (wpow[None, :, :] + 1e-06))


def solution(mesh):
    return jax.shard_map(
        per_device,
        mesh=mesh,
        in_specs=(P("chan", "tm"), P("chan", "tm")),
        out_specs=P("chan", None, "tm"),
        check_vma=False,
    )
```

```python
import math
import functools
import numpy as np
import jax
import jax.numpy as jnp
from jax import lax
from jax.sharding import PartitionSpec as P
from jax.experimental import pallas as pl
from jax.experimental.pallas import tpu as pltpu

NT = (((1,), (1,)), ((), ()))
PITCH = 72


def split(x):
    hi = x.astype(jnp.bfloat16)
    lo = (x - hi.astype(jnp.float32)).astype(jnp.bfloat16)
    return hi, lo


def np_split(x):
    x = jnp.asarray(x, jnp.float32)
    return split(x)


def fft_tables():
    a = np.arange(64)
    ang = 2 * np.pi * np.outer(a, a) % (2 * np.pi * 64) / 64
    ang = 2 * np.pi * (np.outer(a, a) % 64) / 64
    f1 = np.concatenate([np.cos(ang), -np.sin(ang)], 0)
    h, l = np_split(f1)
    f1cat = jnp.concatenate([h, h, l, l], axis=1)
    lane = np.arange(128)
    k2 = np.arange(32)
    ang2 = 2 * np.pi * (np.outer(k2, lane) % 64) / 64
    re = np.concatenate([np.cos(ang2), np.sin(ang2)], 1)
    im = np.concatenate([-np.sin(ang2), np.cos(ang2)], 1)
    h, l = np_split(np.concatenate([re, im], 0))
    w2 = jnp.concatenate([h, l], axis=0)
    k1 = np.arange(128)
    angt = 2 * np.pi * (np.outer(k1, lane) % 8192) / 8192
    cos_t = jnp.asarray(np.cos(angt), jnp.float32)
    sin_t = jnp.asarray(np.sin(angt), jnp.float32)
    n = np.arange(8192)
    hann = jnp.asarray((0.5 - 0.5 * np.cos(2 * np.pi * n / 8192)).reshape(64, 128), jnp.float32)
    return f1cat, w2, cos_t, sin_t, hann


def fft_step(x2d, base, mean8, scr, s, tabs):
    f1, w2, cos_t, sin_t, hann = tabs
    cats = []
    for c in range(8):
        xs = (x2d[pl.ds(base + s * 256 + c, 64, stride=8), :] - mean8[c:c + 1]) * hann[...]
        h, l = split(xs)
        cats.append(jnp.concatenate([h, l, h, l], axis=0))
    y = jnp.dot(f1[...], jnp.concatenate(cats, axis=1), preferred_element_type=jnp.float32)
    zh, zl = [], []
    for c in range(8):
        yre = y[:64, 128 * c:128 * c + 128]
        yim = y[64:, 128 * c:128 * c + 128]
        for b in range(2):
            ct = cos_t[64 * b:64 * b + 64]
            st = sin_t[64 * b:64 * b + 64]
            h, l = split(jnp.concatenate([yre * ct + yim * st, yim * ct - yre * st], axis=1))
            zh.append(h)
            zl.append(l)
    w = w2[...]
    a = lax.dot_general(w, jnp.concatenate(zh, axis=0), NT, preferred_element_type=jnp.float32)
    b = lax.dot_general(w[:64], jnp.concatenate(zl, axis=0), NT, preferred_element_type=jnp.float32)
    o = a[:64] + a[64:] + b
    for c in range(8):
        scr[pl.ds(c * 8 + s, 64, stride=PITCH), :] = o[:, 128 * c:128 * c + 128]


def fused_kernel(peers, aux, wit, f1, w2, cos_t, sin_t, hann, num, apow, wpow,
                 x, scr, send, recv, sums, means, diffs, rows, mat_re, mat_im, wv, eye, numv,
                 load_sem, halo_send, halo_recv, sum_send, sum_recv, send_sem, recv_sem,
                 half_send, half_recv, cross_send, cross_recv, ring_send, ring_recv, out_sem):
    tabs = (f1, w2, cos_t, sin_t, hann)
    mesh_id = pl.DeviceIdType.MESH
    me = lax.axis_index("tm")
    mine = lax.axis_index("chan")
    across = mine + 1 - 2 * lax.rem(mine, 2)
    right = lax.rem(mine + 2, 8)
    left = lax.rem(mine + 6, 8)
    before = lax.rem(me + peers - 1, peers)
    after = lax.rem(me + 1, peers)
    blocks = x.shape[0]
    turn = (blocks + 1) // 2
    slots = send.shape[0]

    def source(b):
        return wit.at[0] if b == 0 else aux.at[b - 1]

    barrier = pltpu.get_barrier_semaphore()

    def greet(j, _):
        to = lax.rem(me + j, peers)
        pl.semaphore_signal(barrier, inc=1, device_id={"tm": to}, device_id_type=mesh_id)
        pl.semaphore_signal(barrier, inc=1, device_id={"tm": to, "chan": across}, device_id_type=mesh_id)
        return 0

    lax.fori_loop(1, peers, greet, 0)
    for c in (across, right, left):
        pl.semaphore_signal(barrier, inc=1, device_id={"chan": c}, device_id_type=mesh_id)
    loads = []
    for b in range(blocks):
        cp = pltpu.make_async_copy(source(b), x.at[b, pl.ds(32 if b >= turn else 0, 256)], load_sem.at[b])
        cp.start()
        loads.append(cp)
    def halo(b, src, late):
        return pltpu.make_async_remote_copy(
            src_ref=src.at[pl.ds(224 if late else 0, 32)], dst_ref=x.at[b, pl.ds(0 if late else 256, 32)],
            send_sem=halo_send.at[b], recv_sem=halo_recv.at[b],
            device_id={"tm": after if late else before}, device_id_type=mesh_id)

    lane = lax.broadcasted_iota(jnp.int32, (8, 128), 1)

    def block_sum(b):
        first = jnp.where(b >= turn, 32, 0)

        def add(i, acc):
            return acc + jnp.sum(x[b, pl.ds(first + i * 32, 32)].reshape(8, 4, 8, 128), axis=0)

        part = jnp.sum(lax.fori_loop(0, 8, add, jnp.zeros((4, 8, 128), jnp.float32)), axis=0)
        total = jnp.sum(part, axis=1, keepdims=True)
        means[b] = jnp.broadcast_to(total / (256 * 128), (8, 128))
        return total

    def sum_copy(r, j):
        return pltpu.make_async_remote_copy(
            src_ref=sums.at[r, 0], dst_ref=sums.at[r, j],
            send_sem=sum_send.at[r, j], recv_sem=sum_recv.at[r, j],
            device_id={"tm": lax.rem(me + j, peers)}, device_id_type=mesh_id)

    def sum_start(r):
        def one(j, _):
            sum_copy(r, j).start()
            return 0
        lax.fori_loop(1, peers, one, 0)

    def total_means(r, which):
        def one(j, acc):
            sum_copy(r, j).wait()
            return acc + sums[r, j]
        total = lax.fori_loop(1, peers, one, sums[r, 0])
        mean = total / (256 * 128 * peers)
        for b in which:
            diffs[b] = means[b] - jnp.broadcast_to(mean[:, b:b + 1], (8, 128))

    loads[0].wait()
    sums[0, 0] = jnp.where(lane == 0, block_sum(0), 0.0)
    pl.semaphore_wait(barrier, 2 * (peers - 1) + 3)
    for b in range(blocks):
        halo(b, source(b), b >= turn).start()
    sum_start(0)
    sums[1, 0] = jnp.zeros((8, 128), jnp.float32)
    eye[...] = (lax.broadcasted_iota(jnp.int32, (128, 128), 0)
                == lax.broadcasted_iota(jnp.int32, (128, 128), 1)).astype(jnp.float32).astype(jnp.bfloat16)

    def other_sum(b):
        pltpu.make_async_copy(aux.at[0], x.at[b, pl.ds(0, 256)], load_sem.at[b]).wait()
        sums[1, 0] = jnp.where(lane == b, block_sum(b), sums[1, 0])

    x2d = x.reshape(blocks * 288 * 8, 128)
    row = lax.broadcasted_iota(jnp.int32, (64, 128), 0)
    keep_next = jnp.where((lax.rem(row, 8) == 7) & (me == peers - 1), 0.0, 1.0)
    keep_last = jnp.where((lax.rem(row, 8) == 0) & (me == 0), 0.0, 1.0)
    col = lax.broadcasted_iota(jnp.int32, (64, 128), 1)
    hann_bins = jnp.where(col == 0, 4096.0, jnp.where(col == 1, -2048.0, 0.0))

    def block_copy(b, j):
        slot = lax.rem(b, slots)
        to = lax.rem(me + 7 * j, peers)
        return pltpu.make_async_remote_copy(
            src_ref=send.at[slot, to], dst_ref=recv.at[b, me],
            send_sem=send_sem.at[slot, j], recv_sem=recv_sem.at[b, j],
            device_id={"tm": to}, device_id_type=mesh_id)

    def drain(b):
        def one(j, _):
            block_copy(b, j).wait_send()
            return 0
        lax.fori_loop(1, peers, one, 0)

    def half_copy(hf, j):
        to = lax.rem(me + 7 * j, peers)
        return pltpu.make_async_remote_copy(
            src_ref=send.at[(blocks - 1) % slots, to, hf], dst_ref=recv.at[blocks - 1, me, hf],
            send_sem=half_send.at[hf, j], recv_sem=half_recv.at[hf, j],
            device_id={"tm": to}, device_id_type=mesh_id)

    def half_wait(hf, send_side):
        def one(j, _):
            if send_side:
                half_copy(hf, j).wait_send()
            else:
                half_copy(hf, j).wait_recv()
            return 0
        lax.fori_loop(1, peers, one, 0)

    def cross_copy(j):
        to = lax.rem(me + 7 * j, peers)
        return pltpu.make_async_remote_copy(
            src_ref=send.at[0, to], dst_ref=recv.at[blocks, me],
            send_sem=cross_send.at[j], recv_sem=cross_recv.at[j],
            device_id={"tm": to, "chan": across}, device_id_type=mesh_id)

    def landed(b):
        def one(j, _):
            block_copy(b, j).wait_recv()
            return 0
        lax.fori_loop(1, peers, one, 0)

    def piece(i, g, lo, n, c):
        return pltpu.make_async_remote_copy(
            src_ref=wv.at[g, pl.ds(lo, n)], dst_ref=wv.at[g, pl.ds(lo, n)],
            send_sem=ring_send.at[i], recv_sem=ring_recv.at[i],
            device_id={"chan": c}, device_id_type=mesh_id)

    frames = wv.shape[1]
    half = frames // 2
    left_across = lax.rem(across + 6, 8)
    right_across = lax.rem(across + 2, 8)
    own_r = piece(0, mine, 0, frames, right)
    own_l = piece(1, mine, 0, frames, left)
    far_r = piece(2, across, 0, frames, right)
    far_l = piece(3, across, 0, frames, left)
    own_rr = piece(4, left, 0, half, right)
    own_ll = piece(5, right, half, half, left)
    far_rr = piece(6, left_across, 0, half, right)
    far_ll = piece(7, right_across, half, half, left)

    def proof_piece(b, g):
        power = []
        for h in range(2):
            gather_rows(recv.at[b], rows, h)
            for w in range(8):
                r = rows[w]
                power.append(jnp.sum(r * r, axis=0, keepdims=True))
                t = flip(eye[...], r)
                mat_re[pl.ds(h * 2048 + w, 128, stride=16), :] = t[:, :128]
                mat_re[pl.ds(h * 2048 + 8 + w, 128, stride=16), :] = t[:, 128:]

        def one(i, _):
            for u in range(8):
                f = i * 8 + u
                wv[g, f] = mat_re[pl.ds(pl.multiple_of(f * 16, 16), 16), :].astype(jnp.bfloat16)
            return 0
        lax.fori_loop(0, 32, one, 0)
        zero = jnp.zeros((8, 128), jnp.float32)
        for h in range(2):
            rest = jnp.concatenate(power[8 * h:8 * h + 8], axis=0)
            for term in range(3):
                top = rest.astype(jnp.bfloat16).astype(jnp.float32)
                wv[g, 256 + 3 * h + term] = jnp.concatenate([top, zero], axis=0).astype(jnp.bfloat16)
                rest = rest - top
        for i in range(262, frames):
            wv[g, i] = jnp.zeros((16, 128), jnp.bfloat16)

    def proof_own():
        landed(0)
        proof_piece(0, mine)
        own_r.start()
        own_l.start()

    def proof_across():
        def one(j, _):
            cross_copy(j).wait_recv()
            return 0
        lax.fori_loop(0, peers, one, 0)
        proof_piece(blocks, across)
        far_r.start()
        far_l.start()

    def aux_half(b, h):
        gather_rows(recv.at[b], rows, h)
        back = jnp.where(b >= turn, 127, 0)
        e = eye[...]
        for c in range(8):
            r = rows[c]
            apow[b - 1, c:c + 1, 128 * h:128 * h + 128] = jnp.sum(r * r, axis=0, keepdims=True)
            t = flip(e, r)
            at = h * 128 * PITCH + (b - 1) * 8 + c
            mat_re[pl.ds(at, 128, stride=PITCH), :] = pltpu.roll(t[:, :128], back, 1)
            mat_im[pl.ds(at, 128, stride=PITCH), :] = pltpu.roll(t[:, 128:], back, 1)

    def aux_block(b):
        landed(b)
        aux_half(b, 0)
        aux_half(b, 1)

    def block(b, _):
        slot = lax.rem(b, slots)
        mean8 = means[b]

        def step(s, _):
            @pl.when((s == 7) & (b < turn))
            def _():
                halo(b, aux.at[0], False).wait()

            @pl.when((s == 0) & (b >= turn))
            def _():
                halo(b, aux.at[0], True).wait()
            fft_step(x2d, b * 2304, mean8, scr, s, tabs)

            @pl.when(b == 0)
            def _():
                other_sum(s + 1)
            return 0

        lax.fori_loop(0, 8, step, 0)

        @pl.when(b == 0)
        def _():
            sum_start(1)
            total_means(0, range(1))

        @pl.when(b == 1)
        def _():
            total_means(1, range(1, blocks))

        @pl.when(b >= slots)
        def _():
            drain(b - slots)

        @pl.when(b == slots)
        def _():
            def one(j, _):
                cross_copy(j).wait_send()
                return 0
            lax.fori_loop(0, peers, one, 0)

        diff = diffs[b]
        shift = jnp.concatenate([jnp.broadcast_to(diff[c:c + 1], (8, 128)) for c in range(8)], axis=0)
        scr[0:64, :] = scr[0:64, :] + shift * hann_bins

        keep = jnp.where(b >= turn, keep_last, keep_next)

        def pack(d, _):
            for part in range(2):
                for hf in range(2):
                    at = pl.multiple_of((part * 32 + d * 2 + hf) * PITCH, 8)
                    v = scr[pl.ds(at, 64), :] * keep
                    send[slot, d, hf, part] = v.astype(jnp.bfloat16)
            return 0

        lax.fori_loop(0, peers, pack, 0)

        @pl.when(b < blocks - 1)
        def _():
            def go(j, _):
                block_copy(b, j).start()
                return 0
            lax.fori_loop(1, peers, go, 0)

        @pl.when(b == blocks - 1)
        def _():
            for hf in range(2):
                def go(j, _):
                    half_copy(hf, j).start()
                    return 0
                lax.fori_loop(1, peers, go, 0)

        recv[b, me] = send[slot, me]

        @pl.when(b == 0)
        def _():
            def cross(j, _):
                cross_copy(j).start()
                return 0
            lax.fori_loop(0, peers, cross, 0)

        @pl.when(b == 1)
        def _():
            proof_own()

        @pl.when(b == 2)
        def _():
            proof_across()

        @pl.when(b >= 3)
        def _():
            aux_block(b - 2)

        @pl.when(b == 5)
        def _():
            own_r.wait_recv()
            own_l.wait_recv()
            own_rr.start()
            own_ll.start()

        @pl.when(b == 7)
        def _():
            far_r.wait_recv()
            far_l.wait_recv()
            far_rr.start()
            far_ll.start()
        return 0

    lax.fori_loop(0, blocks, block, 0)

    def finish(b0, nb, h):
        n = nb * 8

        def bins(i, _):
            got = []
            for u in range(32):
                f = h * 128 + i * 32 + u
                at = pl.ds(pl.multiple_of(f * PITCH + b0 * 8, 8), n)
                lhs = jnp.concatenate([mat_re[at, :], mat_im[at, :]], axis=0).astype(jnp.bfloat16)
                g = lax.dot_general(lhs, wv[:, f].reshape(128, 128), NT, preferred_element_type=jnp.float32)
                p, q = g[:n], g[n:]
                re = p + pltpu.roll(q, 120, 1)
                im = q - pltpu.roll(p, 120, 1)
                mat_re[at, :] = re * re + im * im
            return 0

        lax.fori_loop(0, 4, bins, 0)

        def emit(b, _):
            for c in range(8):
                t = mat_re[pl.ds(h * 128 * PITCH + b * 8 + c, 128, stride=PITCH), :].T
                for g in range(8):
                    numv[b * 8 + c, 8 * g:8 * g + 8, 128 * h:128 * h + 128] = t[16 * g:16 * g + 8]
            return 0

        lax.fori_loop(b0, b0 + nb, emit, 0)

    own_rr.wait_recv()
    own_ll.wait_recv()
    far_rr.wait_recv()
    far_ll.wait_recv()
    for h in range(2):
        for g in range(8):
            v = [wv[g, 256 + 3 * h + term].astype(jnp.float32)[:8] for term in range(3)]
            wpow[8 * g:8 * g + 8, 128 * h:128 * h + 128] = v[0] + v[1] + v[2]
    early = blocks - 3
    for h in range(2):
        finish(0, early, h)

    def out_copy(i, b, n):
        return pltpu.make_async_copy(numv.at[pl.ds(8 * b, 8 * n)], num.at[pl.ds(8 * b, 8 * n)], out_sem.at[i])

    out_copy(0, 0, early).start()
    aux_block(blocks - 2)
    for h in range(2):
        half_wait(h, False)
        aux_half(blocks - 1, h)
        finish(early, 2, h)
    out_copy(1, early, 2).start()
    for cp in (own_r, own_l, far_r, far_l, own_rr, own_ll, far_rr, far_ll):
        cp.wait_send()
    for b in range(blocks - slots, blocks - 1):
        drain(b)
    for h in range(2):
        half_wait(h, True)
    out_copy(0, 0, early).wait()
    out_copy(1, early, 2).wait()


def gather_rows(stage, rows, h):
    def one(t, _):
        for part in range(2):
            v = stage[t, h, part].astype(jnp.float32)
            at = pl.multiple_of(part * 128 + t * 8, 8)
            for c in range(8):
                rows[c, pl.ds(at, 8), :] = v[8 * c:8 * c + 8]
        return 0
    lax.fori_loop(0, 16, one, 0)


def flip(eye, rows_c):
    return lax.dot_general(eye, rows_c.astype(jnp.bfloat16), NT, preferred_element_type=jnp.float32)


def fused(aux, wit, peers):
    tabs = fft_tables()
    vm = pl.BlockSpec(memory_space=pltpu.VMEM)
    hbm = pl.BlockSpec(memory_space=pl.ANY)
    blocks = aux.shape[0] + 1
    slots = 3
    dma = pltpu.SemaphoreType.DMA
    f32, bf16 = jnp.float32, jnp.bfloat16
    return pl.pallas_call(
        functools.partial(fused_kernel, peers),
        out_shape=(jax.ShapeDtypeStruct((64, 64, 256), f32),
                   jax.ShapeDtypeStruct((8, 8, 256), f32),
                   jax.ShapeDtypeStruct((64, 256), f32)),
        in_specs=[hbm, hbm] + [vm] * 5,
        out_specs=(hbm, vm, vm),
        scratch_shapes=[
            pltpu.VMEM((blocks, 288, 8, 128), f32),
            pltpu.VMEM((64 * PITCH, 128), f32),
            pltpu.VMEM((slots, peers, 2, 2, 64, 128), bf16),
            pltpu.VMEM((blocks + 1, peers, 2, 2, 64, 128), bf16),
            pltpu.VMEM((2, peers, 8, 128), f32),
            pltpu.VMEM((blocks, 8, 128), f32),
            pltpu.VMEM((blocks, 8, 128), f32),
            pltpu.VMEM((8, 256, 128), f32),
            pltpu.VMEM((256 * PITCH, 128), f32),
            pltpu.VMEM((256 * PITCH, 128), f32),
            pltpu.VMEM((8, 264, 16, 128), bf16),
            pltpu.VMEM((128, 128), bf16),
            pltpu.VMEM((64, 64, 256), f32),
            dma((blocks,)), dma((blocks,)), dma((blocks,)),
            dma((2, peers)), dma((2, peers)),
            dma((slots, peers)), dma((blocks, peers)),
            dma((2, peers)), dma((2, peers)),
            dma((peers,)), dma((peers,)), dma((8,)), dma((8,)), dma((2,)),
        ],
        compiler_params=pltpu.CompilerParams(
            collective_id=0, has_side_effects=True, vmem_limit_bytes=63 * 2 ** 20),
    )(aux, wit, *tabs)


def divide_kernel(num, apow, wpow, out):
    out[...] = num[...] / ((apow[...][:, None, :] + 1e-06) * (wpow[...][None, :, :] + 1e-06))


def divide(num, apow, wpow):
    rows = 32
    return pl.pallas_call(
        divide_kernel,
        grid=(num.shape[0] // rows,),
        out_shape=jax.ShapeDtypeStruct(num.shape, jnp.float32),
        in_specs=[pl.BlockSpec((rows, 64, 256), lambda i: (i, 0, 0)),
                  pl.BlockSpec((rows, 256), lambda i: (i, 0)),
                  pl.BlockSpec((64, 256), lambda i: (0, 0))],
        out_specs=pl.BlockSpec((rows, 64, 256), lambda i: (i, 0, 0)),
        compiler_params=pltpu.CompilerParams(vmem_limit_bytes=60 * 2 ** 20),
    )(num, apow, wpow)


def tiles(a):
    return a.reshape(a.shape[0] // 8, 8, 256, 128).transpose(0, 2, 1, 3)


def per_device(auxiliary, proofs):
    peers = lax.axis_size("tm")
    num, apow, wpow = fused(tiles(auxiliary), tiles(proofs), peers)
    apow = apow.reshape(64, 256)
    return divide(num, apow, wpow)


def solution(mesh):
    return jax.shard_map(
        per_device,
        mesh=mesh,
        in_specs=(P("chan", "tm"), P("chan", "tm")),
        out_specs=P("chan", None, "tm"),
        check_vma=False,
    )
```

```python
import math
import functools
import numpy as np
import jax
import jax.numpy as jnp
from jax import lax
from jax.sharding import PartitionSpec as P
from jax.experimental import pallas as pl
from jax.experimental.pallas import tpu as pltpu

NT = (((1,), (1,)), ((), ()))
PITCH = 72


def split(x):
    hi = x.astype(jnp.bfloat16)
    lo = (x - hi.astype(jnp.float32)).astype(jnp.bfloat16)
    return hi, lo


def np_split(x):
    x = jnp.asarray(x, jnp.float32)
    return split(x)


def fft_tables():
    a = np.arange(64)
    ang = 2 * np.pi * np.outer(a, a) % (2 * np.pi * 64) / 64
    ang = 2 * np.pi * (np.outer(a, a) % 64) / 64
    f1 = np.concatenate([np.cos(ang), -np.sin(ang)], 0)
    h, l = np_split(f1)
    f1cat = jnp.concatenate([h, h, l, l], axis=1)
    lane = np.arange(128)
    k2 = np.arange(32)
    ang2 = 2 * np.pi * (np.outer(k2, lane) % 64) / 64
    re = np.concatenate([np.cos(ang2), np.sin(ang2)], 1)
    im = np.concatenate([-np.sin(ang2), np.cos(ang2)], 1)
    h, l = np_split(np.concatenate([re, im], 0))
    w2 = jnp.concatenate([h, l], axis=0)
    k1 = np.arange(128)
    angt = 2 * np.pi * (np.outer(k1, lane) % 8192) / 8192
    cos_t = jnp.asarray(np.cos(angt), jnp.float32)
    sin_t = jnp.asarray(np.sin(angt), jnp.float32)
    n = np.arange(8192)
    hann = jnp.asarray((0.5 - 0.5 * np.cos(2 * np.pi * n / 8192)).reshape(64, 128), jnp.float32)
    return f1cat, w2, cos_t, sin_t, hann


def fft_step(x2d, base, mean8, scr, s, tabs):
    f1, w2, cos_t, sin_t, hann = tabs
    cats = []
    for c in range(8):
        xs = (x2d[pl.ds(base + s * 256 + c, 64, stride=8), :] - mean8[c:c + 1]) * hann[...]
        h, l = split(xs)
        cats.append(jnp.concatenate([h, l, h, l], axis=0))
    y = jnp.dot(f1[...], jnp.concatenate(cats, axis=1), preferred_element_type=jnp.float32)
    zh, zl = [], []
    for c in range(8):
        yre = y[:64, 128 * c:128 * c + 128]
        yim = y[64:, 128 * c:128 * c + 128]
        for b in range(2):
            ct = cos_t[64 * b:64 * b + 64]
            st = sin_t[64 * b:64 * b + 64]
            h, l = split(jnp.concatenate([yre * ct + yim * st, yim * ct - yre * st], axis=1))
            zh.append(h)
            zl.append(l)
    w = w2[...]
    a = lax.dot_general(w, jnp.concatenate(zh, axis=0), NT, preferred_element_type=jnp.float32)
    b = lax.dot_general(w[:64], jnp.concatenate(zl, axis=0), NT, preferred_element_type=jnp.float32)
    o = a[:64] + a[64:] + b
    for c in range(8):
        scr[pl.ds(c * 8 + s, 64, stride=PITCH), :] = o[:, 128 * c:128 * c + 128]


def fused_kernel(peers, aux, wit, f1, w2, cos_t, sin_t, hann, num, apow, wpow,
                 x, scr, send, recv, sums, means, diffs, rows, mat_re, mat_im, wv, eye, numv,
                 load_sem, halo_send, halo_recv, sum_send, sum_recv, send_sem, recv_sem,
                 half_send, half_recv, cross_send, cross_recv, ring_send, ring_recv, out_sem):
    tabs = (f1, w2, cos_t, sin_t, hann)
    mesh_id = pl.DeviceIdType.MESH
    me = lax.axis_index("tm")
    mine = lax.axis_index("chan")
    across = mine + 1 - 2 * lax.rem(mine, 2)
    right = lax.rem(mine + 2, 8)
    left = lax.rem(mine + 6, 8)
    before = lax.rem(me + peers - 1, peers)
    after = lax.rem(me + 1, peers)
    blocks = x.shape[0]
    turn = (blocks + 1) // 2
    slots = send.shape[0]

    def source(b):
        return wit.at[0] if b == 0 else aux.at[b - 1]

    barrier = pltpu.get_barrier_semaphore()

    def greet(j, _):
        to = lax.rem(me + j, peers)
        pl.semaphore_signal(barrier, inc=1, device_id={"tm": to}, device_id_type=mesh_id)
        pl.semaphore_signal(barrier, inc=1, device_id={"tm": to, "chan": across}, device_id_type=mesh_id)
        return 0

    lax.fori_loop(1, peers, greet, 0)
    for c in (across, right, left):
        pl.semaphore_signal(barrier, inc=1, device_id={"chan": c}, device_id_type=mesh_id)
    loads = []
    for b in range(blocks):
        cp = pltpu.make_async_copy(source(b), x.at[b, pl.ds(32 if b >= turn else 0, 256)], load_sem.at[b])
        cp.start()
        loads.append(cp)
    def halo(b, src, late):
        return pltpu.make_async_remote_copy(
            src_ref=src.at[pl.ds(224 if late else 0, 32)], dst_ref=x.at[b, pl.ds(0 if late else 256, 32)],
            send_sem=halo_send.at[b], recv_sem=halo_recv.at[b],
            device_id={"tm": after if late else before}, device_id_type=mesh_id)

    lane = lax.broadcasted_iota(jnp.int32, (8, 128), 1)

    def block_sum(b):
        first = jnp.where(b >= turn, 32, 0)

        def add(i, acc):
            return acc + jnp.sum(x[b, pl.ds(first + i * 32, 32)].reshape(8, 4, 8, 128), axis=0)

        part = jnp.sum(lax.fori_loop(0, 8, add, jnp.zeros((4, 8, 128), jnp.float32)), axis=0)
        total = jnp.sum(part, axis=1, keepdims=True)
        means[b] = jnp.broadcast_to(total / (256 * 128), (8, 128))
        return total

    def sum_copy(r, j):
        return pltpu.make_async_remote_copy(
            src_ref=sums.at[r, 0], dst_ref=sums.at[r, j],
            send_sem=sum_send.at[r, j], recv_sem=sum_recv.at[r, j],
            device_id={"tm": lax.rem(me + j, peers)}, device_id_type=mesh_id)

    def sum_start(r):
        def one(j, _):
            sum_copy(r, j).start()
            return 0
        lax.fori_loop(1, peers, one, 0)

    def total_means(r, which):
        def one(j, acc):
            sum_copy(r, j).wait()
            return acc + sums[r, j]
        total = lax.fori_loop(1, peers, one, sums[r, 0])
        mean = total / (256 * 128 * peers)
        for b in which:
            diffs[b] = means[b] - jnp.broadcast_to(mean[:, b:b + 1], (8, 128))

    loads[0].wait()
    sums[0, 0] = jnp.where(lane == 0, block_sum(0), 0.0)
    pl.semaphore_wait(barrier, 2 * (peers - 1) + 3)
    for b in range(blocks):
        halo(b, source(b), b >= turn).start()
    sum_start(0)
    sums[1, 0] = jnp.zeros((8, 128), jnp.float32)
    eye[...] = (lax.broadcasted_iota(jnp.int32, (128, 128), 0)
                == lax.broadcasted_iota(jnp.int32, (128, 128), 1)).astype(jnp.float32).astype(jnp.bfloat16)

    def other_sum(b):
        pltpu.make_async_copy(aux.at[0], x.at[b, pl.ds(0, 256)], load_sem.at[b]).wait()
        sums[1, 0] = jnp.where(lane == b, block_sum(b), sums[1, 0])

    x2d = x.reshape(blocks * 288 * 8, 128)
    row = lax.broadcasted_iota(jnp.int32, (64, 128), 0)
    keep_next = jnp.where((lax.rem(row, 8) == 7) & (me == peers - 1), 0.0, 1.0)
    keep_last = jnp.where((lax.rem(row, 8) == 0) & (me == 0), 0.0, 1.0)
    col = lax.broadcasted_iota(jnp.int32, (64, 128), 1)
    hann_bins = jnp.where(col == 0, 4096.0, jnp.where(col == 1, -2048.0, 0.0))

    def block_copy(b, j):
        slot = lax.rem(b, slots)
        to = lax.rem(me + 7 * j, peers)
        return pltpu.make_async_remote_copy(
            src_ref=send.at[slot, to], dst_ref=recv.at[b, me],
            send_sem=send_sem.at[slot, j], recv_sem=recv_sem.at[b, j],
            device_id={"tm": to}, device_id_type=mesh_id)

    def drain(b):
        def one(j, _):
            block_copy(b, j).wait_send()
            return 0
        lax.fori_loop(1, peers, one, 0)

    def half_copy(hf, j):
        to = lax.rem(me + 7 * j, peers)
        return pltpu.make_async_remote_copy(
            src_ref=send.at[(blocks - 1) % slots, to, hf], dst_ref=recv.at[blocks - 1, me, hf],
            send_sem=half_send.at[hf, j], recv_sem=half_recv.at[hf, j],
            device_id={"tm": to}, device_id_type=mesh_id)

    def half_wait(hf, send_side):
        def one(j, _):
            if send_side:
                half_copy(hf, j).wait_send()
            else:
                half_copy(hf, j).wait_recv()
            return 0
        lax.fori_loop(1, peers, one, 0)

    def cross_copy(j):
        to = lax.rem(me + 7 * j, peers)
        return pltpu.make_async_remote_copy(
            src_ref=send.at[0, to], dst_ref=recv.at[blocks, me],
            send_sem=cross_send.at[j], recv_sem=cross_recv.at[j],
            device_id={"tm": to, "chan": across}, device_id_type=mesh_id)

    def landed(b):
        def one(j, _):
            block_copy(b, j).wait_recv()
            return 0
        lax.fori_loop(1, peers, one, 0)

    def piece(i, g, lo, n, c):
        return pltpu.make_async_remote_copy(
            src_ref=wv.at[g, pl.ds(lo, n)], dst_ref=wv.at[g, pl.ds(lo, n)],
            send_sem=ring_send.at[i], recv_sem=ring_recv.at[i],
            device_id={"chan": c}, device_id_type=mesh_id)

    frames = wv.shape[1]
    half = frames // 2
    left_across = lax.rem(across + 6, 8)
    right_across = lax.rem(across + 2, 8)
    own_r = piece(0, mine, 0, frames, right)
    own_l = piece(1, mine, 0, frames, left)
    far_r = piece(2, across, 0, frames, right)
    far_l = piece(3, across, 0, frames, left)
    own_rr = piece(4, left, 0, half, right)
    own_ll = piece(5, right, half, half, left)
    far_rr = piece(6, left_across, 0, half, right)
    far_ll = piece(7, right_across, half, half, left)

    def proof_piece(b, g):
        power = []
        for h in range(2):
            gather_rows(recv.at[b], rows, h)
            for w in range(8):
                r = rows[w]
                power.append(jnp.sum(r * r, axis=0, keepdims=True))
                t = flip(eye[...], r)
                mat_re[pl.ds(h * 2048 + w, 128, stride=16), :] = t[:, :128]
                mat_re[pl.ds(h * 2048 + 8 + w, 128, stride=16), :] = t[:, 128:]

        def one(i, _):
            for u in range(8):
                f = i * 8 + u
                wv[g, f] = mat_re[pl.ds(pl.multiple_of(f * 16, 16), 16), :].astype(jnp.bfloat16)
            return 0
        lax.fori_loop(0, 32, one, 0)
        zero = jnp.zeros((8, 128), jnp.float32)
        for h in range(2):
            rest = jnp.concatenate(power[8 * h:8 * h + 8], axis=0)
            for term in range(3):
                top = rest.astype(jnp.bfloat16).astype(jnp.float32)
                wv[g, 256 + 3 * h + term] = jnp.concatenate([top, zero], axis=0).astype(jnp.bfloat16)
                rest = rest - top
        for i in range(262, frames):
            wv[g, i] = jnp.zeros((16, 128), jnp.bfloat16)

    def proof_own():
        landed(0)
        proof_piece(0, mine)
        own_r.start()
        own_l.start()

    def proof_across():
        def one(j, _):
            cross_copy(j).wait_recv()
            return 0
        lax.fori_loop(0, peers, one, 0)
        proof_piece(blocks, across)
        far_r.start()
        far_l.start()

    def aux_half(b, h):
        gather_rows(recv.at[b], rows, h)
        back = jnp.where(b >= turn, 127, 0)
        e = eye[...]
        for c in range(8):
            r = rows[c]
            apow[b - 1, c:c + 1, 128 * h:128 * h + 128] = jnp.sum(r * r, axis=0, keepdims=True)
            t = flip(e, r)
            at = h * 128 * PITCH + (b - 1) * 8 + c
            mat_re[pl.ds(at, 128, stride=PITCH), :] = pltpu.roll(t[:, :128], back, 1)
            mat_im[pl.ds(at, 128, stride=PITCH), :] = pltpu.roll(t[:, 128:], back, 1)

    def aux_block(b):
        landed(b)
        aux_half(b, 0)
        aux_half(b, 1)

    def block(b, _):
        slot = lax.rem(b, slots)
        mean8 = means[b]

        def step(s, _):
            @pl.when((s == 7) & (b < turn))
            def _():
                halo(b, aux.at[0], False).wait()

            @pl.when((s == 0) & (b >= turn))
            def _():
                halo(b, aux.at[0], True).wait()
            fft_step(x2d, b * 2304, mean8, scr, s, tabs)

            @pl.when(b == 0)
            def _():
                other_sum(s + 1)
            return 0

        lax.fori_loop(0, 8, step, 0)

        @pl.when(b == 0)
        def _():
            sum_start(1)
            total_means(0, range(1))

        @pl.when(b == 1)
        def _():
            total_means(1, range(1, blocks))

        @pl.when(b >= slots)
        def _():
            drain(b - slots)

        @pl.when(b == slots)
        def _():
            def one(j, _):
                cross_copy(j).wait_send()
                return 0
            lax.fori_loop(0, peers, one, 0)

        diff = diffs[b]
        shift = jnp.concatenate([jnp.broadcast_to(diff[c:c + 1], (8, 128)) for c in range(8)], axis=0)
        scr[0:64, :] = scr[0:64, :] + shift * hann_bins

        keep = jnp.where(b >= turn, keep_last, keep_next)

        def pack(d, _):
            for part in range(2):
                for hf in range(2):
                    at = pl.multiple_of((part * 32 + d * 2 + hf) * PITCH, 8)
                    v = scr[pl.ds(at, 64), :] * keep
                    send[slot, d, hf, part] = v.astype(jnp.bfloat16)
            return 0

        lax.fori_loop(0, peers, pack, 0)

        @pl.when(b < blocks - 1)
        def _():
            def go(j, _):
                block_copy(b, j).start()
                return 0
            lax.fori_loop(1, peers, go, 0)

        @pl.when(b == blocks - 1)
        def _():
            for hf in range(2):
                def go(j, _):
                    half_copy(hf, j).start()
                    return 0
                lax.fori_loop(1, peers, go, 0)

        recv[b, me] = send[slot, me]

        @pl.when(b == 0)
        def _():
            def cross(j, _):
                cross_copy(j).start()
                return 0
            lax.fori_loop(0, peers, cross, 0)

        @pl.when(b == 1)
        def _():
            proof_own()

        @pl.when(b == 2)
        def _():
            proof_across()

        @pl.when(b >= 3)
        def _():
            aux_block(b - 2)

        @pl.when(b == 4)
        def _():
            own_r.wait_recv()
            own_l.wait_recv()
            own_rr.start()
            own_ll.start()

        @pl.when(b == 6)
        def _():
            far_r.wait_recv()
            far_l.wait_recv()
            far_rr.start()
            far_ll.start()
        return 0

    lax.fori_loop(0, blocks, block, 0)

    def finish(b0, nb, h):
        n = nb * 8
        wide = 64 if nb <= 2 else 32

        def bins(i, _):
            for u in range(wide):
                f = h * 128 + i * wide + u
                at = pl.ds(pl.multiple_of(f * PITCH + b0 * 8, 8), n)
                lhs = jnp.concatenate([mat_re[at, :], mat_im[at, :]], axis=0).astype(jnp.bfloat16)
                g = lax.dot_general(lhs, wv[:, f].reshape(128, 128), NT, preferred_element_type=jnp.float32)
                p, q = g[:n], g[n:]
                re = p + pltpu.roll(q, 120, 1)
                im = q - pltpu.roll(p, 120, 1)
                mat_re[at, :] = re * re + im * im
            return 0

        lax.fori_loop(0, 128 // wide, bins, 0)

        def emit(b, _):
            for c in range(8):
                t = mat_re[pl.ds(h * 128 * PITCH + b * 8 + c, 128, stride=PITCH), :].T
                for g in range(8):
                    numv[b * 8 + c, 8 * g:8 * g + 8, 128 * h:128 * h + 128] = t[16 * g:16 * g + 8]
            return 0

        lax.fori_loop(b0, b0 + nb, emit, 0)

    own_rr.wait_recv()
    own_ll.wait_recv()
    far_rr.wait_recv()
    far_ll.wait_recv()
    for h in range(2):
        for g in range(8):
            v = [wv[g, 256 + 3 * h + term].astype(jnp.float32)[:8] for term in range(3)]
            wpow[8 * g:8 * g + 8, 128 * h:128 * h + 128] = v[0] + v[1] + v[2]
    early = blocks - 3
    for h in range(2):
        finish(0, early, h)

    def out_copy(i, b, n):
        return pltpu.make_async_copy(numv.at[pl.ds(8 * b, 8 * n)], num.at[pl.ds(8 * b, 8 * n)], out_sem.at[i])

    out_copy(0, 0, early).start()
    aux_block(blocks - 2)
    for h in range(2):
        half_wait(h, False)
        aux_half(blocks - 1, h)
        finish(early, 2, h)
    out_copy(1, early, 2).start()
    for cp in (own_r, own_l, far_r, far_l, own_rr, own_ll, far_rr, far_ll):
        cp.wait_send()
    for b in range(blocks - slots, blocks - 1):
        drain(b)
    for h in range(2):
        half_wait(h, True)
    out_copy(0, 0, early).wait()
    out_copy(1, early, 2).wait()


def gather_rows(stage, rows, h):
    def one(t, _):
        for part in range(2):
            v = stage[t, h, part].astype(jnp.float32)
            at = pl.multiple_of(part * 128 + t * 8, 8)
            for c in range(8):
                rows[c, pl.ds(at, 8), :] = v[8 * c:8 * c + 8]
        return 0
    lax.fori_loop(0, 16, one, 0)


def flip(eye, rows_c):
    return lax.dot_general(eye, rows_c.astype(jnp.bfloat16), NT, preferred_element_type=jnp.float32)


def fused(aux, wit, peers):
    tabs = fft_tables()
    vm = pl.BlockSpec(memory_space=pltpu.VMEM)
    hbm = pl.BlockSpec(memory_space=pl.ANY)
    blocks = aux.shape[0] + 1
    slots = 3
    dma = pltpu.SemaphoreType.DMA
    f32, bf16 = jnp.float32, jnp.bfloat16
    return pl.pallas_call(
        functools.partial(fused_kernel, peers),
        out_shape=(jax.ShapeDtypeStruct((64, 64, 256), f32),
                   jax.ShapeDtypeStruct((8, 8, 256), f32),
                   jax.ShapeDtypeStruct((64, 256), f32)),
        in_specs=[hbm, hbm] + [vm] * 5,
        out_specs=(hbm, vm, vm),
        scratch_shapes=[
            pltpu.VMEM((blocks, 288, 8, 128), f32),
            pltpu.VMEM((64 * PITCH, 128), f32),
            pltpu.VMEM((slots, peers, 2, 2, 64, 128), bf16),
            pltpu.VMEM((blocks + 1, peers, 2, 2, 64, 128), bf16),
            pltpu.VMEM((2, peers, 8, 128), f32),
            pltpu.VMEM((blocks, 8, 128), f32),
            pltpu.VMEM((blocks, 8, 128), f32),
            pltpu.VMEM((8, 256, 128), f32),
            pltpu.VMEM((256 * PITCH, 128), f32),
            pltpu.VMEM((256 * PITCH, 128), f32),
            pltpu.VMEM((8, 264, 16, 128), bf16),
            pltpu.VMEM((128, 128), bf16),
            pltpu.VMEM((64, 64, 256), f32),
            dma((blocks,)), dma((blocks,)), dma((blocks,)),
            dma((2, peers)), dma((2, peers)),
            dma((slots, peers)), dma((blocks, peers)),
            dma((2, peers)), dma((2, peers)),
            dma((peers,)), dma((peers,)), dma((8,)), dma((8,)), dma((2,)),
        ],
        compiler_params=pltpu.CompilerParams(
            collective_id=0, has_side_effects=True, vmem_limit_bytes=63 * 2 ** 20),
    )(aux, wit, *tabs)


def divide_kernel(num, apow, wpow, out):
    out[...] = num[...] / ((apow[...][:, None, :] + 1e-06) * (wpow[...][None, :, :] + 1e-06))


def divide(num, apow, wpow):
    rows = 32
    return pl.pallas_call(
        divide_kernel,
        grid=(num.shape[0] // rows,),
        out_shape=jax.ShapeDtypeStruct(num.shape, jnp.float32),
        in_specs=[pl.BlockSpec((rows, 64, 256), lambda i: (i, 0, 0)),
                  pl.BlockSpec((rows, 256), lambda i: (i, 0)),
                  pl.BlockSpec((64, 256), lambda i: (0, 0))],
        out_specs=pl.BlockSpec((rows, 64, 256), lambda i: (i, 0, 0)),
        compiler_params=pltpu.CompilerParams(vmem_limit_bytes=60 * 2 ** 20),
    )(num, apow, wpow)


def tiles(a):
    return a.reshape(a.shape[0] // 8, 8, 256, 128).transpose(0, 2, 1, 3)


def per_device(auxiliary, proofs):
    peers = lax.axis_size("tm")
    num, apow, wpow = fused(tiles(auxiliary), tiles(proofs), peers)
    apow = apow.reshape(64, 256)
    return divide(num, apow, wpow)


def solution(mesh):
    return jax.shard_map(
        per_device,
        mesh=mesh,
        in_specs=(P("chan", "tm"), P("chan", "tm")),
        out_specs=P("chan", None, "tm"),
        check_vma=False,
    )
```
